256 devices in a mesh: rep: 4 (over x_lo, core), shard: 64 (over z, x_hi, y).
Axes of the slice: x: 4 (x_hi: 2, x_lo: 2; x = x_hi * 2 + x_lo), y: 4, z: 8, core: 2. Of those that a mesh axis runs over, the one named last changes fastest.
Arguments:
- dense_out: bfloat16 [32768, 128], P(('rep', 'shard')), may hold values from -0.75 to 0.75
- pooled: bfloat16 [32768, 26, 128], P(('rep', 'shard')), may hold values from -0.75 to 0.75
- top_weight: bfloat16 [479, 1024], replicated, may hold values from -0.25 to 0.25
- top_cotangent: bfloat16 [32768, 1024], P(('rep', 'shard')), may hold values from -3 to 3
- indices: int32 [32768, 26, 2], P(('rep', 'shard')), may hold values from 0 to 16383, as said below
Outputs:
- dense_grad: bfloat16 [32768, 128], P(('rep', 'shard'))
- top_grad: float32 [479, 1024], replicated
- bias_grad: float32 [1024], replicated
- table_grad: float32 [26, 16384, 128], P(None, 'shard')
The draws below stay inside these ranges and needn't reach their ends.
Inputs may be any that keep to these rules, and one draw needn't show every extreme that they name: `indices`: rows r with r // 256 = s are held by shard s. For every device's 128 samples and every table, at most 2 of the device's lookups fall in any one block of 64 rows starting at a multiple of 64, and some such block holds exactly 2.
All inputs are finite; a program needn't handle non-finite values.
Results may differ from the reference program's by a relative error of at most 0.008.
Values may be sent and summed in bfloat16 or wider, within the bound.
A program may use at most 128 MiB of HBM per device.

```python
import jax
import jax.numpy as jnp
import numpy as np
from jax import lax

E = 128
F = 26
H = 1024
B_DEV = 128
L = 2
R_SHARD = 256
IN = 479
BATCH = 32768
ROWS = 16384
N_REP = 4
N_SHARD = 64


def draw_indices(key, part):
    devices_all = N_REP * N_SHARD
    blocks = N_SHARD * N_REP
    per_block = 2 * B_DEV * L // blocks
    lookups = B_DEV * L
    row_span = R_SHARD // N_REP
    places = blocks * per_block

    def draw_bag(subkey):
        key_full, key_order, key_offset, key_shuffle = jax.random.split(subkey, 4)
        full_block = jax.random.randint(key_full, (), 0, blocks, dtype=jnp.int32)
        place_ids = jnp.arange(places, dtype=jnp.int32)
        ranking = jax.random.permutation(key_order, places).astype(jnp.int32)
        scores = jnp.where(place_ids // per_block == full_block, place_ids - places, ranking)
        chosen = jnp.argsort(scores, stable=True)[:lookups].astype(jnp.int32)
        offsets = jax.random.randint(key_offset, (lookups,), 0, row_span, dtype=jnp.int32)
        rows_drawn = chosen // per_block * row_span + offsets
        shuffle = jax.random.permutation(key_shuffle, lookups)
        return rows_drawn[shuffle].reshape(B_DEV, L)
    subkeys = jax.random.split(key, devices_all * F)
    drawn_rows = jax.vmap(draw_bag)(subkeys).reshape(devices_all, F, B_DEV, L)
    return jnp.transpose(drawn_rows, (0, 2, 1, 3)).reshape(devices_all * B_DEV, F, L).astype(jnp.int32)


def steps_of(rng, extent, shards, smallest, high):
    factor_of, own = 1.0, jax.random.fold_in(rng, 6)
    for position, blocks in shards:
        draws = jnp.exp(jax.random.uniform(jax.random.fold_in(own, position), (blocks,), jnp.float32, smallest / len(shards), high / len(shards)))
        factor_of = factor_of * jnp.repeat(draws, extent[position] // blocks).reshape([-1 if axis == position else 1 for axis in range(len(extent))])
    return factor_of


def bell_draw(rng, shape, deviation, bound, pieces=(), held_as=jnp.bfloat16):
    factor_of = steps_of(rng, shape, pieces, -0.22, 0.18) if pieces else 1.0
    array = jax.random.normal(rng, shape, jnp.float32) * deviation * factor_of
    return jnp.minimum(jnp.maximum(array, -bound), bound).astype(held_as)


def setup_inputs(seed: int = 0) -> dict:
    keys = jax.random.split(jax.random.key(seed), 6)
    return {
        "dense_out": bell_draw(keys[0], (BATCH, E), 0.125, 0.75, ((0, 256),)),
        "pooled": bell_draw(keys[1], (BATCH, F, E), 0.125, 0.75, ((0, 256),)),
        "top_weight": bell_draw(keys[2], (IN, H), IN ** -0.5, 0.25),
        "top_cotangent": bell_draw(keys[3], (BATCH, H), 0.5, 3.0, ((0, 256),)),
        "indices": draw_indices(jax.random.fold_in(keys[5], 71), 0),
    }


highest = lax.Precision.HIGHEST


def reference(dense_out, pooled, top_weight, top_cotangent, indices):
    vectors = F + 1
    lower_i, lower_j = np.tril_indices(vectors, -1)
    blocks = BATCH // B_DEV
    table_index = jnp.arange(F, dtype=jnp.int32)

    def block_step(totals, inputs):
        top_acc, bias_acc, table_acc = totals
        dense_block, pooled_block, cot_block, index_block = inputs
        stacked = jnp.concatenate([dense_block[:, None, :], pooled_block], axis=1).astype(jnp.float32)
        gram_matrix = jnp.einsum("bie,bje->bij", stacked, stacked, precision=highest)
        pair_values = gram_matrix[:, lower_i, lower_j].astype(jnp.bfloat16)
        joined = jnp.concatenate([dense_block, pair_values], axis=1)
        grad_in = jnp.dot(cot_block, top_weight.T, preferred_element_type=jnp.float32)
        top_acc = top_acc + jnp.dot(joined.T, cot_block, preferred_element_type=jnp.float32)
        bias_acc = bias_acc + jnp.sum(cot_block.astype(jnp.float32), axis=0)
        pair_grad = grad_in[:, E:]
        mirror = jnp.zeros((pair_grad.shape[0], vectors, vectors), jnp.float32)
        mirror = mirror.at[:, lower_i, lower_j].set(pair_grad)
        mirror = mirror.at[:, lower_j, lower_i].set(pair_grad)
        vec_grad = jnp.einsum("bij,bje->bie", mirror, stacked, precision=highest)
        dense_grad = (grad_in[:, :E] + vec_grad[:, 0]).astype(jnp.bfloat16)
        pooled_grad = vec_grad[:, 1:].astype(jnp.bfloat16)
        updates = jnp.broadcast_to(pooled_grad.astype(jnp.float32)[:, :, None, :], (B_DEV, F, L, E))
        table_acc = table_acc.at[table_index[None, :, None], index_block].add(updates)
        return (top_acc, bias_acc, table_acc), dense_grad

    start = (jnp.zeros((IN, H), jnp.float32), jnp.zeros((H,), jnp.float32), jnp.zeros((F, ROWS, E), jnp.float32))
    inputs = (dense_out.reshape(blocks, B_DEV, E), pooled.reshape(blocks, B_DEV, F, E), top_cotangent.reshape(blocks, B_DEV, H), indices.reshape(blocks, B_DEV, F, L))
    totals, dense_parts = lax.scan(block_step, start, inputs)
    top_grad, bias_grad, table_grad = totals
    return dense_parts.reshape(BATCH, E), top_grad, bias_grad, table_grad
```

```python
import functools

import jax
import jax.numpy as jnp
from jax import lax
from jax.experimental import pallas as pl
from jax.experimental.pallas import tpu as pltpu
from jax.sharding import PartitionSpec as P

F32=jnp.float32; BF=jnp.bfloat16
NT=(((1,),(1,)),((),()))
def coords():
    r=lax.axis_index("rep"); s=lax.axis_index("shard")
    return (s//4)%2*2+r//2, s%4, s//8, r%2
def local_kernel(dense, pooled, w, cot, idx, dgrad, top, rows, vt, g, gt, cd, kacc):
    x,y,z,c=coords()
    i0=lax.broadcasted_iota(jnp.int32,(128,128),0); i1=lax.broadcasted_iota(jnp.int32,(128,128),1)
    eye=(i0==i1).astype(F32).astype(BF)
    vt[0]=lax.dot_general(eye,dense[...],NT,preferred_element_type=F32)
    def tr(i,_):
        vt[i+1]=lax.dot_general(eye,pooled[i],NT,preferred_element_type=F32)
        return 0
    lax.fori_loop(0,26,tr,0,unroll=2)
    gt[0:479]=lax.dot_general(w[...],cot[...],NT,preferred_element_type=F32)
    gt[479:480]=jnp.zeros((1,128),F32)
    g[0:128]=vt[0]
    g[479:480]=jnp.ones((1,128),F32)
    def prow(a,b):
        hi=jnp.maximum(a,b); lo=jnp.minimum(a,b)
        return 128+hi*(hi-1)//2+lo
    def gram(i,_):
        va=vt[i]
        for d in range(1,14):
            j=i+d
            j=jnp.where(j>=27,j-27,j)
            s=jnp.sum(va*vt[j],axis=0,keepdims=True)
            g[pl.ds(prow(i,j),1),:]=s
        return 0
    lax.fori_loop(0,27,gram,0)
    top[...]=jnp.dot(g[...].astype(BF),cot[...],preferred_element_type=F32).astype(top.dtype)
    blk=idx[...]//64
    sh=idx[...]//256
    j4=blk-sh*4
    z_=sh//8; xh=(sh//4)%2; y_=sh%4
    x_=xh*2+j4//2; c_=j4%2
    slot=(((x_^x)*4+(y_^y))*2+(c_^c))*16+((z_-z+8)%8)*2
    key=idx[...]%64+1
    cd[0:26]=blk.astype(F32)
    cd[26:52]=slot.astype(F32)
    cd[52:78]=key.astype(F32)
    kacc[...]=jnp.zeros_like(kacc)
    lt=i0<i1
    s512=lax.broadcasted_iota(jnp.int32,(512,128),0).astype(F32)
    def dense_out(_):
        pass
    def vg(i):
        acc=jnp.zeros((128,128),F32)
        for j in range(27):
            p=jnp.where(i==j,479,prow(i,jnp.int32(j)))
            acc=acc+gt[pl.ds(p,1),:]*vt[j]
        return acc
    d0=vg(jnp.int32(0))+gt[0:128]
    dgrad[...]=lax.dot_general(eye,d0.astype(BF),NT,preferred_element_type=F32).astype(BF)
    def table(t,_):
        v=vg(t+1).astype(BF)
        b=cd[t]
        bt=jnp.concatenate([b,jnp.zeros((126,128),F32)],axis=0).T
        c0=bt[:,0:1]; c1=bt[:,1:2]
        one=jnp.float32(1); zero=jnp.float32(0)
        r0=jnp.sum(jnp.where((c0==b[0:1])&lt,one,zero),axis=0,keepdims=True)
        r1=jnp.sum(jnp.where(c0==b[1:2],one,zero)+jnp.where((c1==b[1:2])&lt,one,zero),axis=0,keepdims=True)
        sl=cd[t+26]
        P0=jnp.where(s512==sl[0:1]+r0,one,zero).astype(BF)
        P1=jnp.where(s512==sl[1:2]+r1,one,zero).astype(BF)
        P=jnp.concatenate([P0,P1],axis=1)
        kv=cd[t+52]
        R=jnp.where(i0==t,kv[0:1],zero).astype(BF); R1=jnp.where(i0==t,kv[1:2],zero).astype(BF)
        rhs=jnp.concatenate([jnp.concatenate([v,v],axis=1),jnp.concatenate([R,R1],axis=1)],axis=0)
        o=lax.dot_general(P,rhs,NT,preferred_element_type=F32)
        rows[t+1]=o[:,0:128].astype(BF)
        kacc[...]+=o[:,128:256]
        return 0
    lax.fori_loop(0,26,table,0)
    rows[0]=kacc[...].astype(BF)

def local_call(dense, pooled_t, w, cot, idx_t):
    vm=pl.BlockSpec(memory_space=pltpu.VMEM)
    return pl.pallas_call(local_kernel,
        out_shape=(jax.ShapeDtypeStruct((128,128),BF),jax.ShapeDtypeStruct((480,1024),F32),jax.ShapeDtypeStruct((27,512,128),BF)),
        in_specs=[vm]*5,out_specs=(vm,)*3,
        scratch_shapes=[pltpu.VMEM((27,128,128),F32),pltpu.VMEM((480,128),F32),pltpu.VMEM((480,128),F32),pltpu.VMEM((78,2,128),F32),pltpu.VMEM((512,128),F32)],
        compiler_params=pltpu.CompilerParams(vmem_limit_bytes=40*2**20),name="local")(dense,pooled_t,w,cot,idx_t)

MESH=pl.DeviceIdType.MESH
T=3; NC=9; E=T*NC
def xor4(a,b):
    al=a%2; ah=a//2; bl=b%2; bh=b//2
    return ((ah+bh)%2)*2+(al+bl)%2
def dev(x,y,z,c):
    return ((x%2)*2+c, z*8+(x//2)*4+y)
def plane_peer(q):
    x,y,z,c=coords()
    return dev(xor4(x,q//8),xor4(y,(q//2)%4),z,(c+q)%2)
def z_peer(d):
    x,y,z,c=coords()
    return dev(x,y,(z+d+8)%8,c)
def rep_peer(i):
    x,y,z,c=coords()
    r=(x%2)*2+c
    return (xor4(r,i), z*8+(x//2)*4+y)
def comm_kernel(rows, out, rv, kt, D, zr, fin, s_send, s_recv, z_send, z_recv, a_send, a_recv):
    bar=pltpu.get_barrier_semaphore()
    def sig(q,_):
        pl.semaphore_signal(bar,1,device_id=plane_peer(q),device_id_type=MESH)
        return 0
    lax.fori_loop(1,32,sig,0)
    for d in (1,-1):
        pl.semaphore_signal(bar,1,device_id=z_peer(d),device_id_type=MESH)
    pl.semaphore_wait(bar,33)
    def s_chunk(ch,_):
        def s_one(q,_):
            pltpu.make_async_remote_copy(src_ref=rows.at[pl.ds(ch*T,T),pl.ds(q*16,16)],dst_ref=rv.at[pl.ds(ch*T,T),pl.ds(q*16,16)],
               send_sem=s_send.at[ch],recv_sem=s_recv.at[ch],device_id=plane_peer(q),device_id_type=MESH).start()
            return 0
        lax.fori_loop(1,32,s_one,0)
        return 0
    lax.fori_loop(0,NC,s_chunk,0)
    def zcopy(dirn, step, ch):
        rel=(5-step) if dirn==0 else (3+step)
        if step==1:
            lo=32*dirn; sz=32
        else:
            lo=0; sz=64
        return pltpu.make_async_remote_copy(
            src_ref=D.at[pl.ds(ch*T,T),rel,pl.ds(lo,sz)],dst_ref=zr.at[dirn,step-1,pl.ds(ch*T,T),pl.ds(lo,sz)],
            send_sem=z_send.at[dirn,step-1,ch],recv_sem=z_recv.at[dirn,step-1,ch],
            device_id=z_peer(1 if dirn==0 else -1),device_id_type=MESH)
    def acopy(i,ch):
        r=lax.axis_index("rep")
        return pltpu.make_async_remote_copy(
            src_ref=fin.at[pl.ds(ch*T,T)],dst_ref=out.at[pl.ds(ch*T,T),pl.ds(pl.multiple_of(r*64,64),64)],
            send_sem=a_send.at[i-1,ch],recv_sem=a_recv.at[i-1,ch],device_id=rep_peer(i),device_id_type=MESH)
    rowi=lax.broadcasted_iota(jnp.int32,(512,512),0).astype(F32)
    def step(k,_):
        @pl.when(k<NC)
        def _():
            ch=k
            reg=rv.at[pl.ds(ch*T,T),pl.ds(16,496)]
            pltpu.make_async_copy(reg,reg,s_recv.at[ch]).wait()
            rv[pl.ds(ch*T,T),0:16]=rows[pl.ds(ch*T,T),0:16]
            @pl.when(ch==0)
            def _():
                i0=lax.broadcasted_iota(jnp.int32,(128,128),0); i1=lax.broadcasted_iota(jnp.int32,(128,128),1)
                eye=(i0==i1).astype(F32).astype(BF)
                kk=lax.dot_general(eye,rv[0],NT,preferred_element_type=F32)
                zz=(lax.broadcasted_iota(jnp.int32,(128,512),1)%16//2*64).astype(F32)
                kt[...]=jnp.where(kk>0.5,kk-1+zz,-1.0)
            def acc(t,_):
                e=ch*T+t
                kr=kt[pl.ds((e+127)%128,1),:]
                oh=jnp.where(rowi==kr,jnp.float32(1),jnp.float32(0)).astype(BF)
                d=jnp.dot(oh,rv[e],preferred_element_type=F32).astype(BF)
                D[e]=d.reshape(8,64,128)
                return 0
            lax.fori_loop(0,T,acc,0)
            zcopy(0,1,ch).start(); zcopy(1,1,ch).start()
        for s in (1,2,3):
            @pl.when((k>=s)&(k<NC+s))
            def _(s=s):
                ch=k-s
                for dirn in (0,1):
                    zcopy(dirn,s,ch).wait_recv()
                    rel=(4-s) if dirn==0 else (4+s)
                    lo,sz=(32*dirn,32) if s==1 else (0,64)
                    for t in range(T):
                        e=ch*T+t
                        D[e,rel,lo:lo+sz]=(D[e,rel,lo:lo+sz].astype(F32)+zr[dirn,s-1,e,lo:lo+sz].astype(F32)).astype(BF)
                    zcopy(dirn,s+1,ch).start()
        @pl.when((k>=4)&(k<NC+4))
        def _():
            ch=k-4
            r=lax.axis_index("rep")
            zcopy(0,4,ch).wait_recv(); zcopy(1,4,ch).wait_recv()
            for t in range(T):
                e=ch*T+t
                v=(D[e,0].astype(F32)+zr[0,3,e].astype(F32)+zr[1,3,e].astype(F32)).astype(BF)
                fin[e]=v
                out[e,pl.ds(pl.multiple_of(r*64,64),64)]=v
            for i in (1,2,3): acopy(i,ch).start()
        return 0
    lax.fori_loop(0,NC+4,step,0)
    def drain(ch,_):
        for i in (1,2,3):
            acopy(i,ch).wait()
        for dirn in (0,1):
            for s in (1,2,3,4): zcopy(dirn,s,ch).wait_send()
        reg=rows.at[pl.ds(ch*T,T),pl.ds(16,496)]
        pltpu.make_async_copy(reg,reg,s_send.at[ch]).wait()
        return 0
    lax.fori_loop(0,NC,drain,0)

def comm_call(rows):
    vm=pl.BlockSpec(memory_space=pltpu.VMEM)
    return pl.pallas_call(comm_kernel,out_shape=jax.ShapeDtypeStruct((E,256,128),BF),in_specs=[vm],out_specs=vm,
      scratch_shapes=[pltpu.VMEM((E,512,128),BF),pltpu.VMEM((128,512),F32),pltpu.VMEM((E,8,64,128),BF),pltpu.VMEM((2,4,E,64,128),BF),pltpu.VMEM((E,64,128),BF),
        pltpu.SemaphoreType.DMA((NC,)),pltpu.SemaphoreType.DMA((NC,)),
        pltpu.SemaphoreType.DMA((2,4,NC)),pltpu.SemaphoreType.DMA((2,4,NC)),pltpu.SemaphoreType.DMA((3,NC)),pltpu.SemaphoreType.DMA((3,NC))],
      compiler_params=pltpu.CompilerParams(collective_id=1,has_side_effects=True,vmem_limit_bytes=56*2**20),name="comm")(rows)

def on_device(dense_out, pooled, top_weight, top_cotangent, indices):
    dgrad, top, rows = local_call(dense_out, jnp.transpose(pooled,(1,0,2)), top_weight, top_cotangent, jnp.transpose(indices,(1,2,0)))
    table = comm_call(rows)
    top = lax.psum(top, ("rep", "shard"))
    return dgrad, top[:479], top[479], table[1:].astype(F32)


def solution(mesh):
    both = P(("rep", "shard"))
    return jax.shard_map(on_device, mesh=mesh, in_specs=(both, both, P(), both, both),
        out_specs=(both, P(), P(), P(None, "shard", None)), check_vma=False)
```

```python
import jax
import jax.numpy as jnp
from jax import lax
from jax.experimental import pallas as pl
from jax.experimental.pallas import tpu as pltpu
F32 = jnp.float32
BF = jnp.bfloat16
NT = (((1,), (1,)), ((), ()))
MESH = pl.DeviceIdType.MESH
SIZES = (2, 3, 3, 3, 3, 3, 3, 3, 3)
NC = len(SIZES)
STARTS = tuple(sum(SIZES[:i]) for i in range(NC))
NT_ = 26
AHEAD = 3
HOOK = (1, 3, 5, 6, 9)
RELAY = True


def coords():
    r = lax.axis_index("rep")
    s = lax.axis_index("shard")
    return (s // 4) % 2 * 2 + r // 2, s % 4, s // 8, r % 2


def xor4(a, b):
    return ((a // 2 + b // 2) % 2) * 2 + (a % 2 + b % 2) % 2


def dev(x, y, z, c):
    return ((x % 2) * 2 + c, z * 8 + (x // 2) * 4 + y)


def plane_peer(q):
    x, y, z, c = coords()
    return dev(xor4(x, q // 8), xor4(y, (q // 2) % 4), z, (c + q) % 2)


def z_peer(d):
    x, y, z, c = coords()
    return dev(x, y, (z + d + 8) % 8, c)


def rep_peer(i):
    x, y, z, c = coords()
    return (xor4((x % 2) * 2 + c, i), z * 8 + (x // 2) * 4 + y)


def rcopy(src, dst, ss, rs, to):
    return pltpu.make_async_remote_copy(
        src_ref=src, dst_ref=dst, send_sem=ss, recv_sem=rs, device_id=to, device_id_type=MESH)


def kernel(dense_h, pool_h, w_h, cot_h, idx_h, dgrad, topo, bias, tab,
           dense, pool, w, cot, idx, vt, g, gt, sl, cs, keyt, krow, krv, kt,
           rows, rv, D, zr, fin, tb, tp, r0, h, r1, s1, r2, f64,
           in_sem, s_send, s_recv, z_send, z_recv, a_send, a_recv, t_send, t_recv):
    x, y, z, c = coords()
    rep = (x % 2) * 2 + c
    ins = [pltpu.make_async_copy(a, b, in_sem.at[i]) for i, (a, b) in enumerate(
        ((idx_h, idx), (pool_h, pool), (dense_h, dense), (cot_h, cot), (w_h, w)))]
    for cp in ins:
        cp.start()
    bar = pltpu.get_barrier_semaphore()

    def sig(q, _):
        pl.semaphore_signal(bar, 1, device_id=plane_peer(q), device_id_type=MESH)
        return 0

    lax.fori_loop(1, 32, sig, 0)

    def sigz(d, _):
        pl.semaphore_signal(bar, 1, device_id=z_peer(d), device_id_type=MESH)
        return 0

    lax.fori_loop(1, 8, sigz, 0)
    i0 = lax.broadcasted_iota(jnp.int32, (128, 128), 0)
    i1 = lax.broadcasted_iota(jnp.int32, (128, 128), 1)
    eye = (i0 == i1).astype(F32).astype(BF)
    one = jnp.float32(1)
    zero = jnp.float32(0)

    ins[0].wait()
    cs[...] = jnp.zeros_like(cs)
    keyt[...] = jnp.zeros_like(keyt)
    keys, slots, blks = [], [], []
    for l in range(2):
        row = idx[:, l, :]
        blk = row // 64
        sh = row // 256
        part = blk - sh * 4
        xx = (sh // 4) % 2 * 2 + part // 2
        slot = ((xor4(xx, x) * 4 + xor4(sh % 4, y)) * 2 + (part + c) % 2) * 16 + ((sh // 8 - z + 8) % 8) * 2
        keys.append((row - blk * 64 + 1).astype(F32))
        slots.append(slot.astype(F32))
        cs[32 * l:32 * l + 26] = blk.astype(F32)
    ct = cs[...].T
    ltf = jnp.where(i0 < i1, one, zero)
    for t in range(NT_):
        c0 = ct[:, t:t + 1]
        c1 = ct[:, 32 + t:33 + t]
        b0 = cs[t:t + 1]
        b1 = cs[32 + t:33 + t]
        sl[0, t:t + 1] = jnp.sum(jnp.where(c0 == b0, ltf, zero), axis=0, keepdims=True)
        sl[1, t:t + 1] = jnp.sum(jnp.where(c0 == b1, one, zero) + jnp.where(c1 == b1, ltf, zero), axis=0, keepdims=True)
    for l in range(2):
        s = sl[l] + slots[l]
        sl[l] = s
        cs[32 * l:32 * l + 26] = s
        cs[64 + 32 * l:90 + 32 * l] = keys[l]
    ct = cs[...].T
    l512 = lax.broadcasted_iota(jnp.int32, (128, 512), 1).astype(F32)
    for t in range(NT_):
        m = jnp.where(ct[:, t:t + 1] == l512, ct[:, 64 + t:65 + t], zero)
        m = m + jnp.where(ct[:, 32 + t:33 + t] == l512, ct[:, 96 + t:97 + t], zero)
        keyt[t:t + 1] = jnp.sum(m, axis=0, keepdims=True)
    krow[...] = keyt[...].T.astype(BF)

    ins[1].wait()
    ins[2].wait()
    vt[0] = lax.dot_general(eye, dense[...], NT, preferred_element_type=F32)

    def tr(i, _):
        vt[i + 1] = lax.dot_general(eye, pool[i], NT, preferred_element_type=F32)
        return 0

    lax.fori_loop(0, NT_, tr, 0, unroll=2)
    ins[3].wait()
    ins[4].wait()
    gt[0:479] = lax.dot_general(w[...], cot[...], NT, preferred_element_type=F32)
    gt[479:480] = jnp.zeros((1, 128), F32)

    pl.semaphore_wait(bar, 38)

    def k_one(q, _):
        rcopy(krow.at[pl.ds(q * 16, 16)], krv.at[pl.ds(q * 16, 16)], s_send.at[NC], s_recv.at[NC], plane_peer(q)).start()
        return 0

    lax.fori_loop(1, 32, k_one, 0)

    def prow(a, b):
        hi = jnp.maximum(a, b)
        lo = jnp.minimum(a, b)
        return 128 + hi * (hi - 1) // 2 + lo

    def vg(i):
        acc = jnp.zeros((128, 128), F32)
        for j in range(27):
            p = jnp.where(i == j, 479, prow(i, jnp.int32(j)))
            acc = acc + gt[pl.ds(p, 1), :] * vt[j]
        return acc

    s512 = lax.broadcasted_iota(jnp.int32, (512, 128), 0).astype(F32)

    def compute(ch):
        t0, n = STARTS[ch], SIZES[ch]

        def table(t, _):
            v = vg(t + 1).astype(BF)
            s0 = sl[0, pl.ds(t, 1), :]
            s1_ = sl[1, pl.ds(t, 1), :]
            p = jnp.where((s512 == s0) , one, zero) + jnp.where(s512 == s1_, one, zero)
            rows[t] = lax.dot_general(p.astype(BF), v, NT, preferred_element_type=F32).astype(BF)
            return 0

        lax.fori_loop(t0, t0 + n, table, 0)

        def s_one(q, _):
            rcopy(rows.at[pl.ds(t0, n), pl.ds(q * 16, 16)], rv.at[pl.ds(t0, n), pl.ds(q * 16, 16)],
                  s_send.at[ch], s_recv.at[ch], plane_peer(q)).start()
            return 0

        lax.fori_loop(1, 32, s_one, 0)

    def top_part():
        g[0:128] = vt[0]
        g[479:480] = jnp.ones((1, 128), F32)

        def gram(i, _):
            va = vt[i]
            for d in range(1, 14):
                j = i + d
                j = jnp.where(j >= 27, j - 27, j)
                g[pl.ds(prow(i, j), 1), :] = jnp.sum(va * vt[j], axis=0, keepdims=True)
            return 0

        lax.fori_loop(0, 27, gram, 0)
        gb = g[...].astype(BF)
        for i in range(2):
            tp[i, 0:480] = jnp.dot(gb, cot[:, 512 * i:512 * i + 512], preferred_element_type=F32).astype(BF)
            tp[i, 480:512] = jnp.zeros((32, 512), BF)

    def core_copy():
        return rcopy(tp.at[1 - c], r0, t_send.at[0], t_recv.at[0], rep_peer(1))

    def z_share(d):
        zz = (z + d) % 8
        return rcopy(h.at[pl.ds(pl.multiple_of(zz * 64, 64), 64)], r1.at[d - 1], t_send.at[1], t_recv.at[1], z_peer(d))

    def spot(ref, xx, yy):
        return ref.at[pl.ds(pl.multiple_of(xx * 16, 16), 16), pl.ds(pl.multiple_of(yy * 128, 128), 128)]

    def p_share(q):
        return rcopy(spot(s1, xor4(x, q // 4), xor4(y, q % 4)), r2.at[q - 1], t_send.at[2], t_recv.at[2], plane_peer(q * 2))

    def p_gather(q):
        return rcopy(spot(f64, x, y), spot(f64, x, y), t_send.at[3], t_recv.at[3], plane_peer(q * 2))

    def z_gather(d):
        reg = tb.at[c, pl.ds(pl.multiple_of(z * 64, 64), 64)]
        return rcopy(f64, reg, t_send.at[4], t_recv.at[4], z_peer(d))

    def core_gather():
        return rcopy(tb.at[c], tb.at[c], t_send.at[5], t_recv.at[5], rep_peer(1))

    def each(n, copy):
        def one_(i, _):
            copy(i).start()
            return 0
        lax.fori_loop(1, n, one_, 0)

    def wait_for(reg, sem):
        pltpu.make_async_copy(reg, reg, sem).wait()

    def hook0():
        core_copy().wait_recv()
        h[...] = (tp[c].astype(F32) + r0[...].astype(F32)).astype(BF)
        each(8, z_share)

    def hook1():
        wait_for(r1, t_recv.at[1])
        a = h[pl.ds(pl.multiple_of(z * 64, 64), 64)].astype(F32)
        for i in range(7):
            a = a + r1[i].astype(F32)
        s1[...] = a.astype(BF)
        each(16, p_share)

    def hook2():
        wait_for(r2, t_recv.at[2])
        a = spot(s1, x, y)[...].astype(F32)
        for i in range(15):
            a = a + r2[i].astype(F32)
        spot(f64, x, y)[...] = a.astype(BF)
        each(16, p_gather)

    def hook3():
        wait_for(r2, t_recv.at[3])
        tb[c, pl.ds(pl.multiple_of(z * 64, 64), 64)] = f64[...]
        each(8, z_gather)

    def hook4():
        wait_for(r1, t_recv.at[4])
        core_gather().start()

    hooks = dict(zip(HOOK, (hook0, hook1, hook2, hook3, hook4)))

    def zcopy(dirn, step, ch):
        t0, n = STARTS[ch], SIZES[ch]
        rel = (5 - step) if dirn == 0 else (3 + step)
        lo, sz = (32 * dirn, 32) if step == 1 else (0, 64)
        return rcopy(D.at[pl.ds(t0, n), rel, pl.ds(lo, sz)], zr.at[dirn, step - 1, pl.ds(t0, n), pl.ds(lo, sz)],
                     z_send.at[dirn, step - 1, ch], z_recv.at[dirn, step - 1, ch], z_peer(1 if dirn == 0 else -1))

    def acopy(i, ch):
        t0, n = STARTS[ch], SIZES[ch]
        reg = fin.at[pl.ds(t0, n), pl.ds(pl.multiple_of(rep * 64, 64), 64)]
        return rcopy(reg, reg, a_send.at[i - 1, ch], a_recv.at[i - 1, ch], rep_peer(i))

    def fwd(ch):
        t0, n = STARTS[ch], SIZES[ch]
        reg = fin.at[pl.ds(t0, n), pl.ds(pl.multiple_of((rep + 2) % 4 * 64, 64), 64)]
        return rcopy(reg, reg, a_send.at[2, ch], a_recv.at[2, ch], rep_peer(1))

    rowi = lax.broadcasted_iota(jnp.int32, (512, 512), 0).astype(F32)

    def gather_rows(ch):
        t0, n = STARTS[ch], SIZES[ch]
        if ch == 0:
            wait_for(krv.at[pl.ds(16, 496)], s_recv.at[NC])
            krv[0:16] = krow[0:16]
            kk = lax.dot_general(eye, krv[...], NT, preferred_element_type=F32)
            zz = (lax.broadcasted_iota(jnp.int32, (128, 512), 1) % 16 // 2 * 64).astype(F32)
            kt[...] = jnp.where(kk > 0.5, kk - 1 + zz, -1.0)
        wait_for(rv.at[pl.ds(t0, n), pl.ds(16, 496)], s_recv.at[ch])
        rv[t0:t0 + n, 0:16] = rows[t0:t0 + n, 0:16]

        def acc(t, _):
            oh = jnp.where(rowi == kt[pl.ds(t, 1), :], one, zero).astype(BF)
            D[t] = jnp.dot(oh, rv[t], preferred_element_type=F32).astype(BF).reshape(8, 64, 128)
            return 0

        lax.fori_loop(t0, t0 + n, acc, 0)
        zcopy(0, 1, ch).start()
        zcopy(1, 1, ch).start()

    def zstep(s, ch):
        t0, n = STARTS[ch], SIZES[ch]
        for dirn in (0, 1):
            zcopy(dirn, s, ch).wait_recv()
            rel = (4 - s) if dirn == 0 else (4 + s)
            lo, sz = (32 * dirn, 32) if s == 1 else (0, 64)
            for e in range(t0, t0 + n):
                D[e, rel, lo:lo + sz] = (D[e, rel, lo:lo + sz].astype(F32) + zr[dirn, s - 1, e, lo:lo + sz].astype(F32)).astype(BF)
            zcopy(dirn, s + 1, ch).start()

    def finish(ch):
        t0, n = STARTS[ch], SIZES[ch]
        zcopy(0, 4, ch).wait_recv()
        zcopy(1, 4, ch).wait_recv()
        for e in range(t0, t0 + n):
            v = D[e, 0].astype(F32) + zr[0, 3, e].astype(F32) + zr[1, 3, e].astype(F32)
            fin[e, pl.ds(pl.multiple_of(rep * 64, 64), 64)] = v.astype(BF)
        acopy(1, ch).start()
        acopy(2, ch).start()
        if not RELAY:
            acopy(3, ch).start()

    compute(0)
    top_part()
    core_copy().start()
    for ch in range(1, AHEAD):
        compute(ch)
    for k in range(NC + 4):
        if k + AHEAD < NC:
            compute(k + AHEAD)
        if k == NC - AHEAD:
            d0 = vg(jnp.int32(0)) + gt[0:128]
            dgrad[...] = lax.dot_general(eye, d0.astype(BF), NT, preferred_element_type=F32).astype(BF)
        if 0 <= k - 4 < NC:
            finish(k - 4)
        for s in (3, 2, 1):
            if 0 <= k - s < NC:
                zstep(s, k - s)
        if k < NC:
            gather_rows(k)
        if k in hooks:
            hooks[k]()
    if RELAY:
        for ch in range(NC):
            acopy(2, ch).wait_recv()
            fwd(ch).start()
    core_gather().wait_recv()
    for i in range(2):
        topo[:, 512 * i:512 * i + 512] = tb[i, 0:479].astype(F32)
        bias[:, 512 * i:512 * i + 512] = tb[i, 479:480].astype(F32)
    for ch in range(NC):
        t0, n = STARTS[ch], SIZES[ch]
        acopy(1, ch).wait_recv()
        if RELAY:
            fwd(ch).wait_recv()
        else:
            acopy(2, ch).wait_recv()
            acopy(3, ch).wait_recv()
        tab[t0:t0 + n] = fin[t0:t0 + n].astype(F32)
    for ch in range(NC):
        t0, n = STARTS[ch], SIZES[ch]
        acopy(1, ch).wait_send()
        acopy(2, ch).wait_send()
        if RELAY:
            fwd(ch).wait_send()
        else:
            acopy(3, ch).wait_send()
        for dirn in (0, 1):
            for s in (1, 2, 3, 4):
                zcopy(dirn, s, ch).wait_send()
        wait_for(rows.at[pl.ds(t0, n), pl.ds(16, 496)], s_send.at[ch])
    wait_for(krow.at[pl.ds(16, 496)], s_send.at[NC])
    core_copy().wait_send()
    wait_for(r1, t_send.at[1])
    wait_for(r2, t_send.at[2])
    wait_for(r2, t_send.at[3])
    wait_for(r1, t_send.at[4])
    core_gather().wait_send()


def fused_call(dense, pool, w, cot, idx, cid=1, name="fused"):
    vm = pl.BlockSpec(memory_space=pltpu.VMEM)
    hbm = pl.BlockSpec(memory_space=pltpu.HBM)
    dma = pltpu.SemaphoreType.DMA
    V = pltpu.VMEM
    return pl.pallas_call(
        kernel,
        out_shape=(
            jax.ShapeDtypeStruct((128, 128), BF),
            jax.ShapeDtypeStruct((479, 1024), F32),
            jax.ShapeDtypeStruct((1, 1024), F32),
            jax.ShapeDtypeStruct((26, 256, 128), F32),
        ),
        in_specs=[hbm] * 5,
        out_specs=(vm,) * 4,
        scratch_shapes=[
            V((128, 128), BF), V((26, 128, 128), BF), V((479, 1024), BF), V((128, 1024), BF), V((26, 2, 128), jnp.int32),
            V((27, 128, 128), F32), V((480, 128), F32), V((480, 128), F32), V((2, 26, 128), F32), V((128, 128), F32),
            V((128, 512), F32), V((512, 128), BF), V((512, 128), BF), V((128, 512), F32),
            V((26, 512, 128), BF), V((26, 512, 128), BF), V((26, 8, 64, 128), BF), V((2, 4, 26, 64, 128), BF), V((26, 256, 128), BF),
            V((2, 512, 512), BF), V((2, 512, 512), BF), V((512, 512), BF), V((512, 512), BF), V((7, 64, 512), BF),
            V((64, 512), BF), V((15, 16, 128), BF), V((64, 512), BF),
            dma((5,)), dma((NC + 1,)), dma((NC + 1,)), dma((2, 4, NC)), dma((2, 4, NC)), dma((3, NC)), dma((3, NC)), dma((6,)), dma((6,)),
        ],
        compiler_params=pltpu.CompilerParams(collective_id=cid, has_side_effects=True, vmem_limit_bytes=40 * 2**20),
        name=name,
    )(dense, pool, w, cot, idx)


def on_device(dense_out, pooled, top_weight, top_cotangent, indices):
    dgrad, top, bias, table = fused_call(
        dense_out, jnp.transpose(pooled, (1, 0, 2)), top_weight, top_cotangent, jnp.transpose(indices, (1, 2, 0)))
    return dgrad, top, bias.reshape(1024), table


def solution(mesh):
    from jax.sharding import PartitionSpec as P
    both = P(("rep", "shard"))
    return jax.shard_map(
        on_device, mesh=mesh, in_specs=(both, both, P(), both, both),
        out_specs=(both, P(), P(), P(None, "shard", None)), check_vma=False)
```

```python
import contextlib

import jax
import jax.numpy as jnp
from jax import lax
from jax.experimental import pallas as pl
from jax.experimental.pallas import tpu as pltpu
from jax.sharding import PartitionSpec as P

F32 = jnp.float32
BF = jnp.bfloat16
NT = (((1,), (1,)), ((), ()))
MESH = pl.DeviceIdType.MESH
TABLES = 26
SIZES = (2,) * 13
NC = len(SIZES)
STARTS = tuple(sum(SIZES[:i]) for i in range(NC))
AHEAD = 3
LAG = 2
TOP_AT = -1
HOOKS = {"share": 8, "gather_z": 10, "gather_p": 12, "gather_c": 15}
DIRECT = (NC - 1,)
def scope(name):
    return contextlib.nullcontext()


def coords():
    r = lax.axis_index("rep")
    s = lax.axis_index("shard")
    return (s // 4) % 2 * 2 + r // 2, s % 4, s // 8, r % 2


def plane_peer(q):
    x, y, z, c = coords()
    xl = (x + q // 8) % 2
    xh = (x // 2 + q // 16) % 2
    yy = (y // 2 + q // 4) % 2 * 2 + (y + q // 2) % 2
    return (xl * 2 + (c + q) % 2, z * 8 + xh * 4 + yy)


def z_peer(d):
    return (lax.axis_index("rep"), (lax.axis_index("shard") + 8 * d + 64) % 64)


def rep_peer(i):
    r = lax.axis_index("rep")
    return ((r // 2 + i // 2) % 2 * 2 + (r + i) % 2, lax.axis_index("shard"))


def rcopy(src, dst, ss, rs, to):
    return pltpu.make_async_remote_copy(
        src_ref=src, dst_ref=dst, send_sem=ss, recv_sem=rs, device_id=to, device_id_type=MESH)


def wait_for(reg, sem):
    pltpu.make_async_copy(reg, reg, sem).wait()


def kernel(dense_h, pool_h, w_h, cot_h, idx_h, dgrad, topo, bias, tab,
           dense, pool, w, cot, idx, vt, g, gt, sl, cols, keyt, krow, krv, kt,
           rows, rv, D, zr, fin, tb, tp, r0, s1, r2, pz,
           in_sem, s_send, s_recv, z_send, z_recv, a_send, a_recv, t_send, t_recv):
    x, y, z, c = coords()
    rep = lax.axis_index("rep")
    ins = [pltpu.make_async_copy(a, b, in_sem.at[i]) for i, (a, b) in enumerate(
        ((idx_h, idx), (pool_h, pool), (dense_h, dense), (cot_h, cot), (w_h, w)))]
    for cp in ins:
        cp.start()
    bar = pltpu.get_barrier_semaphore()
    with scope("bar"):
        for q in range(1, 32):
            pl.semaphore_signal(bar, 1, device_id=plane_peer(q), device_id_type=MESH)
        for d in range(1, 8):
            pl.semaphore_signal(bar, 1, device_id=z_peer(d), device_id_type=MESH)
    i0 = lax.broadcasted_iota(jnp.int32, (128, 128), 0)
    i1 = lax.broadcasted_iota(jnp.int32, (128, 128), 1)
    eye = (i0 == i1).astype(F32).astype(BF)
    one = jnp.float32(1)
    zero = jnp.float32(0)

    with scope("in0"):
        ins[0].wait()
    with scope("slots"):
        cols[...] = jnp.zeros_like(cols)
        keys, slots = [], []
        for l in range(2):
            row = idx[:, l, :]
            blk = row >> 6
            xx = ((row >> 10) & 1) * 2 + ((row >> 7) & 1)
            slot = ((xx ^ x) << 7) + ((((row >> 8) & 3) ^ y) << 5) + ((((row >> 6) & 1) ^ c) << 4)
            slot = slot + ((((row >> 11) - z) & 7) << 1)
            keys.append(((row & 63) + 1).astype(F32))
            slots.append(slot.astype(F32))
            cols[32 * l:32 * l + 26] = blk.astype(F32)
            sl[l] = blk.astype(F32)
        ct = cols[...].T
    with scope("rank"):
        sub = lax.broadcasted_iota(jnp.int32, (8, 128), 0)
        lane = lax.broadcasted_iota(jnp.int32, (8, 128), 1)
        for t in range(TABLES):
            b0 = jnp.broadcast_to(sl[0, t:t + 1], (8, 128))
            b1 = jnp.broadcast_to(sl[1, t:t + 1], (8, 128))
            n0 = jnp.zeros((8, 128), F32)
            n1 = n0
            for k in range(16):
                c0 = jnp.broadcast_to(ct[8 * k:8 * k + 8, t:t + 1], (8, 128))
                c1 = jnp.broadcast_to(ct[8 * k:8 * k + 8, 32 + t:33 + t], (8, 128))
                lt = jnp.where(sub + 8 * k < lane, one, zero)
                n0 = n0 + jnp.where(c0 == b0, lt, zero)
                n1 = n1 + jnp.where(c0 == b1, one, zero) + jnp.where(c1 == b1, lt, zero)
            cols[64 + t:65 + t] = jnp.sum(n0, axis=0, keepdims=True)
            cols[96 + t:97 + t] = jnp.sum(n1, axis=0, keepdims=True)
        for l in range(2):
            sl[l] = slots[l] + cols[64 + 32 * l:90 + 32 * l]

    def send_keys():
        for l in range(2):
            cols[32 * l:32 * l + 26] = sl[l]
            cols[64 + 32 * l:90 + 32 * l] = keys[l]
        ct = cols[...].T
        fl = lax.broadcasted_iota(jnp.int32, (8, 128), 1).astype(F32)
        lanes = [fl + jnp.float32(128 * b) for b in range(4)]
        keyt[...] = jnp.zeros_like(keyt)
        for t in range(TABLES):
            acc = [jnp.zeros((8, 128), F32)] * 4
            for k in range(16):
                col = [jnp.broadcast_to(ct[8 * k:8 * k + 8, 32 * j + t:32 * j + t + 1], (8, 128)) for j in range(4)]
                for b in range(4):
                    acc[b] = acc[b] + jnp.where(col[0] == lanes[b], col[2], zero) + jnp.where(col[1] == lanes[b], col[3], zero)
            for b in range(4):
                keyt[t:t + 1, 128 * b:128 * b + 128] = jnp.sum(acc[b], axis=0, keepdims=True)
        krow[...] = keyt[...].T.astype(BF)
        for q in range(1, 32):
            rcopy(krow.at[pl.ds(q * 16, 16)], krv.at[pl.ds(q * 16, 16)], s_send.at[NC], s_recv.at[NC], plane_peer(q)).start()

    with scope("in1"):
        ins[1].wait()
        ins[2].wait()
    with scope("tr"):
        vt[0] = lax.dot_general(eye, dense[...], NT, preferred_element_type=F32)

        def tr(i, _):
            vt[i + 1] = lax.dot_general(eye, pool[i], NT, preferred_element_type=F32)
            return 0

        lax.fori_loop(0, TABLES, tr, 0, unroll=2)
    with scope("in3"):
        ins[3].wait()
        ins[4].wait()
    with scope("gt"):
        gt[0:479] = lax.dot_general(w[...], cot[...], NT, preferred_element_type=F32)
        gt[479:480] = jnp.zeros((1, 128), F32)
    with scope("barwait"):
        pl.semaphore_wait(bar, 38)

    def prow(a, b):
        hi = jnp.maximum(a, b)
        lo = jnp.minimum(a, b)
        return 128 + hi * (hi - 1) // 2 + lo

    def vg(i):
        acc = jnp.zeros((128, 128), F32)
        for j in range(27):
            p = jnp.where(i == j, 479, prow(i, jnp.int32(j)))
            acc = acc + gt[pl.ds(p, 1), :] * vt[j]
        return acc

    s512 = lax.broadcasted_iota(jnp.int32, (512, 128), 0).astype(F32)

    def compute(ch):
        t0, n = STARTS[ch], SIZES[ch]

        def table(t, _):
            v = vg(t + 1).astype(BF)
            p = jnp.where((s512 == sl[0, pl.ds(t, 1), :]) | (s512 == sl[1, pl.ds(t, 1), :]), one, zero)
            rows[t] = lax.dot_general(p.astype(BF), v, NT, preferred_element_type=F32).astype(BF)
            return 0

        lax.fori_loop(t0, t0 + n, table, 0)
        for q in range(1, 32):
            rcopy(rows.at[pl.ds(t0, n), pl.ds(q * 16, 16)], rv.at[pl.ds(t0, n), pl.ds(q * 16, 16)],
                  s_send.at[ch], s_recv.at[ch], plane_peer(q)).start()

    def dense_part():
        d0 = vg(jnp.int32(0)) + gt[0:128]
        dgrad[...] = lax.dot_general(eye, d0.astype(BF), NT, preferred_element_type=F32).astype(BF)

    def core_copy():
        return rcopy(tp.at[1 - c], r0, t_send.at[0], t_recv.at[0], rep_peer(1))

    def top_part():
        g[0:128] = vt[0]
        g[479:480] = jnp.ones((1, 128), F32)

        def gram(i, _):
            va = vt[i]
            for d in range(1, 14):
                j = i + d
                j = jnp.where(j >= 27, j - 27, j)
                g[pl.ds(prow(i, j), 1), :] = jnp.sum(va * vt[j], axis=0, keepdims=True)
            return 0

        lax.fori_loop(0, 27, gram, 0)
        gb = g[...].astype(BF)
        for i in range(2):
            tp[i, 0:480] = jnp.dot(gb, cot[:, 512 * i:512 * i + 512], preferred_element_type=F32).astype(BF)
            tp[i, 480:512] = jnp.zeros((32, 512), BF)
        core_copy().start()

    def top_sum():
        core_copy().wait_recv()
        for k in range(8):
            at = pl.ds(pl.multiple_of((z + k) % 8 * 64, 64), 64)
            v = (tp[c, at].astype(F32) + r0[at].astype(F32)).astype(BF)
            for b in range(4):
                D[TABLES + b, k] = v[:, 128 * b:128 * b + 128]
        zcopy(0, 1, NC).start()
        zcopy(1, 1, NC).start()

    def spot(ref, xx, yy):
        return ref.at[yy, pl.ds(pl.multiple_of(xx * 16, 16), 16)]

    def p_target(q):
        return (x // 2 + q // 8) % 2 * 2 + (x + q // 4) % 2, (y // 2 + q // 2) % 2 * 2 + (y + q) % 2

    def p_share(q):
        return rcopy(spot(s1, *p_target(q)), r2.at[q - 1], t_send.at[2], t_recv.at[2], plane_peer(q * 2))

    def z_gather(d):
        return rcopy(pz, tb.at[c, x * 4 + y, z], t_send.at[3], t_recv.at[3], z_peer(d))

    def p_gather(q):
        reg = tb.at[c, x * 4 + y]
        return rcopy(reg, reg, t_send.at[4], t_recv.at[4], plane_peer(q * 2))

    def core_gather():
        return rcopy(tb.at[c], tb.at[c], t_send.at[5], t_recv.at[5], rep_peer(1))

    def top_share():
        zcopy(0, 4, NC).wait_recv()
        zcopy(1, 4, NC).wait_recv()
        for b in range(4):
            e = TABLES + b
            s1[b] = (D[e, 0].astype(F32) + zr[0, 3, e].astype(F32) + zr[1, 3, e].astype(F32)).astype(BF)
        for q in range(1, 16):
            p_share(q).start()

    def top_gather_z():
        wait_for(r2, t_recv.at[2])
        a = spot(s1, x, y)[...].astype(F32)
        for i in range(15):
            a = a + r2[i].astype(F32)
        pz[...] = a.astype(BF)
        tb[c, x * 4 + y, z] = a.astype(BF)
        for d in range(1, 8):
            z_gather(d).start()

    def top_gather_p():
        wait_for(r2.at[pl.ds(0, 7)], t_recv.at[3])
        for q in range(1, 16):
            p_gather(q).start()

    def top_gather_c():
        wait_for(tb.at[0, pl.ds(0, 15)], t_recv.at[4])
        core_gather().start()

    def span(ch):
        return (STARTS[ch], SIZES[ch]) if ch < NC else (TABLES, 4)

    def zcopy(dirn, step, ch):
        t0, n = span(ch)
        rel = (5 - step) if dirn == 0 else (3 + step)
        lo, sz = (32 * dirn, 32) if step == 1 else (0, 64)
        return rcopy(D.at[pl.ds(t0, n), rel, pl.ds(lo, sz)], zr.at[dirn, step - 1, pl.ds(t0, n), pl.ds(lo, sz)],
                     z_send.at[dirn, step - 1, ch], z_recv.at[dirn, step - 1, ch], z_peer(1 if dirn == 0 else -1))

    def acopy(i, ch):
        t0, n = STARTS[ch], SIZES[ch]
        reg = fin.at[pl.ds(t0, n), pl.ds(pl.multiple_of(rep * 64, 64), 64)]
        return rcopy(reg, reg, a_send.at[i - 1, ch], a_recv.at[i - 1, ch], rep_peer(i))

    def fwd(ch):
        t0, n = STARTS[ch], SIZES[ch]
        reg = fin.at[pl.ds(t0, n), pl.ds(pl.multiple_of((rep + 2) % 4 * 64, 64), 64)]
        return rcopy(reg, reg, a_send.at[2, ch], a_recv.at[2, ch], rep_peer(1))

    def third(ch):
        return acopy(3, ch) if ch in DIRECT else fwd(ch)

    rowi = lax.broadcasted_iota(jnp.int32, (512, 512), 0).astype(F32)

    def gather_keys():
        wait_for(krv.at[pl.ds(16, 496)], s_recv.at[NC])
        krv[0:16] = krow[0:16]
        kk = lax.dot_general(eye, krv[...], NT, preferred_element_type=F32)
        zz = (((lax.broadcasted_iota(jnp.int32, (128, 512), 1) >> 1) & 7) << 6).astype(F32)
        kt[...] = jnp.where(kk > 0.5, kk - 1 + zz, -1.0)

    def gather_rows(ch):
        t0, n = STARTS[ch], SIZES[ch]
        wait_for(rv.at[pl.ds(t0, n), pl.ds(16, 496)], s_recv.at[ch])
        rv[t0:t0 + n, 0:16] = rows[t0:t0 + n, 0:16]

        def acc(t, _):
            oh = jnp.where(rowi == kt[pl.ds(t, 1), :], one, zero).astype(BF)
            D[t] = jnp.dot(oh, rv[t], preferred_element_type=F32).astype(BF).reshape(8, 64, 128)
            return 0

        lax.fori_loop(t0, t0 + n, acc, 0)
        zcopy(0, 1, ch).start()
        zcopy(1, 1, ch).start()

    def zstep(s, ch):
        t0, n = span(ch)
        for dirn in (0, 1):
            zcopy(dirn, s, ch).wait_recv()
            rel = (4 - s) if dirn == 0 else (4 + s)
            lo, sz = (32 * dirn, 32) if s == 1 else (0, 64)
            for e in range(t0, t0 + n):
                D[e, rel, lo:lo + sz] = (D[e, rel, lo:lo + sz].astype(F32) + zr[dirn, s - 1, e, lo:lo + sz].astype(F32)).astype(BF)
            zcopy(dirn, s + 1, ch).start()

    def finish(ch):
        t0, n = STARTS[ch], SIZES[ch]
        zcopy(0, 4, ch).wait_recv()
        zcopy(1, 4, ch).wait_recv()
        for e in range(t0, t0 + n):
            v = D[e, 0].astype(F32) + zr[0, 3, e].astype(F32) + zr[1, 3, e].astype(F32)
            fin[e, pl.ds(pl.multiple_of(rep * 64, 64), 64)] = v.astype(BF)
        acopy(1, ch).start()
        acopy(2, ch).start()
        if ch in DIRECT:
            acopy(3, ch).start()

    def named(name, f, *args):
        with scope(name):
            f(*args)

    chain = list(range(NC))
    chain.insert(TOP_AT + 1, NC)
    named("comp", compute, 0)
    named("comp", compute, 1)
    named("keys", send_keys)
    named("comp", compute, 2)
    named("top", top_part)
    made = AHEAD
    steps = len(chain) + 4 * LAG
    extra = {v: k for k, v in HOOKS.items()}
    acts = {"share": top_share, "gather_z": top_gather_z, "gather_p": top_gather_p, "gather_c": top_gather_c}
    for k in range(max(steps, max(extra) + 1)):
        if made < NC:
            named("comp", compute, made)
            made += 1
        elif made == NC:
            named("dense", dense_part)
            made += 1
        for s in (4, 3, 2, 1):
            i = k - LAG * s
            if 0 <= i < len(chain):
                ch = chain[i]
                if s < 4:
                    named("zs%d_%d" % (s, ch), zstep, s, ch)
                elif ch < NC:
                    named("fin%d" % ch, finish, ch)
        if k < len(chain):
            if chain[k] == NC:
                named("tsum", top_sum)
            else:
                if chain[k] == 0:
                    named("gkeys", gather_keys)
                named("gath%d" % chain[k], gather_rows, chain[k])
        if k in extra:
            named(extra[k], acts[extra[k]])
    with scope("fwd"):
        for ch in range(NC):
            if ch not in DIRECT:
                acopy(2, ch).wait_recv()
                fwd(ch).start()
    with scope("topw"):
        core_gather().wait_recv()
        for cc in range(2):
            for xx in range(4):
                for yy in range(4):
                    for zz in range(8):
                        r, q = zz * 64 + xx * 16, cc * 512 + yy * 128
                        if r < 464:
                            topo[r:r + 16, q:q + 128] = tb[cc, xx * 4 + yy, zz].astype(F32)
                        elif r == 464:
                            v = tb[cc, xx * 4 + yy, zz].astype(F32)
                            topo[r:r + 15, q:q + 128] = v[0:15]
                            bias[q // 128:q // 128 + 1] = v[15:16]
    with scope("tabw"):
        for ch in range(NC):
            t0, n = STARTS[ch], SIZES[ch]
            acopy(1, ch).wait_recv()
            if ch in DIRECT:
                acopy(2, ch).wait_recv()
            third(ch).wait_recv()
            tab[t0:t0 + n] = fin[t0:t0 + n].astype(F32)
    with scope("drain"):
        for ch in range(NC):
            t0, n = STARTS[ch], SIZES[ch]
            acopy(1, ch).wait_send()
            acopy(2, ch).wait_send()
            third(ch).wait_send()
            wait_for(rows.at[pl.ds(t0, n), pl.ds(16, 496)], s_send.at[ch])
        for ch in range(NC + 1):
            for dirn in (0, 1):
                for s in (1, 2, 3, 4):
                    zcopy(dirn, s, ch).wait_send()
        wait_for(krow.at[pl.ds(16, 496)], s_send.at[NC])
        core_copy().wait_send()
        wait_for(r2, t_send.at[2])
        wait_for(r2.at[pl.ds(0, 7)], t_send.at[3])
        wait_for(tb.at[0, pl.ds(0, 15)], t_send.at[4])
        core_gather().wait_send()


def fused_call(dense, pool, w, cot, idx, cid=1, name="fused"):
    vm = pl.BlockSpec(memory_space=pltpu.VMEM)
    hbm = pl.BlockSpec(memory_space=pltpu.HBM)
    dma = pltpu.SemaphoreType.DMA
    V = pltpu.VMEM
    E = TABLES + 4
    return pl.pallas_call(
        kernel,
        out_shape=(
            jax.ShapeDtypeStruct((128, 128), BF),
            jax.ShapeDtypeStruct((479, 1024), F32),
            jax.ShapeDtypeStruct((8, 128), F32),
            jax.ShapeDtypeStruct((TABLES, 256, 128), F32),
        ),
        in_specs=[hbm] * 5,
        out_specs=(vm,) * 4,
        scratch_shapes=[
            V((128, 128), BF), V((TABLES, 128, 128), BF), V((479, 1024), BF), V((128, 1024), BF), V((TABLES, 2, 128), jnp.int32),
            V((27, 128, 128), F32), V((480, 128), F32), V((480, 128), F32), V((2, TABLES, 128), F32), V((128, 128), F32),
            V((128, 512), F32), V((512, 128), BF), V((512, 128), BF), V((128, 512), F32),
            V((TABLES, 512, 128), BF), V((TABLES, 512, 128), BF), V((E, 8, 64, 128), BF), V((2, 4, E, 64, 128), BF),
            V((TABLES, 256, 128), BF),
            V((2, 16, 8, 16, 128), BF), V((2, 512, 512), BF), V((512, 512), BF), V((4, 64, 128), BF), V((15, 16, 128), BF), V((16, 128), BF),
            dma((5,)), dma((NC + 1,)), dma((NC + 1,)), dma((2, 4, NC + 1)), dma((2, 4, NC + 1)), dma((3, NC)), dma((3, NC)), dma((6,)), dma((6,)),
        ],
        compiler_params=pltpu.CompilerParams(collective_id=cid, has_side_effects=True, vmem_limit_bytes=40 * 2**20),
        name=name,
    )(*[pltpu.with_memory_space_constraint(a, pltpu.HBM) for a in (dense, pool, w, cot, idx)])


def result_kernel(dgrad, topo, bias, tab, dgrad_o, topo_o, bias_o, tab_o, sem):
    pairs = [(tab.at[pl.ds(i, 2)], tab_o.at[pl.ds(i, 2)]) for i in range(0, TABLES, 2)]
    pairs += [(topo.at[pl.ds(i, 120)], topo_o.at[pl.ds(i, 120)]) for i in (0, 120, 240)]
    pairs += [(topo.at[pl.ds(360, 119)], topo_o.at[pl.ds(360, 119)]), (dgrad, dgrad_o), (bias, bias_o)]
    copies = [pltpu.make_async_copy(a, b, sem.at[i]) for i, (a, b) in enumerate(pairs)]
    for cp in copies:
        cp.start()
    for cp in copies:
        cp.wait()


def result_call(*arrays):
    vm = pl.BlockSpec(memory_space=pltpu.VMEM)
    hbm = pl.BlockSpec(memory_space=pltpu.HBM)
    return pl.pallas_call(
        result_kernel, out_shape=tuple(jax.ShapeDtypeStruct(a.shape, a.dtype) for a in arrays),
        in_specs=[vm] * 4, out_specs=(hbm,) * 4, scratch_shapes=[pltpu.SemaphoreType.DMA((19,))],
        compiler_params=pltpu.CompilerParams(vmem_limit_bytes=2**20), name="result")(*arrays)


def on_device(dense_out, pooled, top_weight, top_cotangent, indices):
    dgrad, top, bias, table = fused_call(
        dense_out, jnp.transpose(pooled, (1, 0, 2)), top_weight, top_cotangent, jnp.transpose(indices, (1, 2, 0)))
    dgrad, top, bias, table = result_call(dgrad, top, bias, table)
    return dgrad, top, bias.reshape(1024), table


def solution(mesh):
    both = P(("rep", "shard"))
    return jax.shard_map(
        on_device, mesh=mesh, in_specs=(both, both, P(), both, both),
        out_specs=(both, P(), P(), P(None, "shard", None)), check_vma=False)
```

```python
import contextlib

import jax
import jax.numpy as jnp
from jax import lax
from jax.experimental import pallas as pl
from jax.experimental.pallas import tpu as pltpu
from jax.sharding import PartitionSpec as P

F32 = jnp.float32
BF = jnp.bfloat16
NT = (((1,), (1,)), ((), ()))
MESH = pl.DeviceIdType.MESH
TABLES = 26
SIZES = (2,) * 13
NC = len(SIZES)
STARTS = tuple(sum(SIZES[:i]) for i in range(NC))
AHEAD = 3
LAG = 2
TOP_AT = -1
HOOKS = {"share": 8, "gather_z": 12, "gather_p": 15, "gather_c": 21}
RELAYED = NC - 1
TR = STARTS[RELAYED]
REST = 2 * TR + 3 * (TABLES - TR)
def scope(name):
    return contextlib.nullcontext()


def coords():
    r = lax.axis_index("rep")
    s = lax.axis_index("shard")
    return (s // 4) % 2 * 2 + r // 2, s % 4, s // 8, r % 2


def plane_peer(q):
    x, y, z, c = coords()
    xl = (x + q // 8) % 2
    xh = (x // 2 + q // 16) % 2
    yy = (y // 2 + q // 4) % 2 * 2 + (y + q // 2) % 2
    return (xl * 2 + (c + q) % 2, z * 8 + xh * 4 + yy)


def z_peer(d):
    return (lax.axis_index("rep"), (lax.axis_index("shard") + 8 * d + 64) % 64)


def rep_peer(i):
    r = lax.axis_index("rep")
    return ((r // 2 + i // 2) % 2 * 2 + (r + i) % 2, lax.axis_index("shard"))


def rcopy(src, dst, ss, rs, to):
    return pltpu.make_async_remote_copy(
        src_ref=src, dst_ref=dst, send_sem=ss, recv_sem=rs, device_id=to, device_id_type=MESH)


def wait_for(reg, sem):
    pltpu.make_async_copy(reg, reg, sem).wait()


def kernel(dense_h, pool_h, w_h, cot_h, idx_h, dgrad, topo, bias, tab,
           dense, pool, w, cot, idx, vt, g, gt, sl, cols, keyt, krow, krv, kt,
           rows, rv, D, zr, fin, tb, tp, r0, s1, r2, pz,
           in_sem, s_send, k_send, s_recv, z_send, z_recv, a_send, a_recv, t_send, t_recv):
    x, y, z, c = coords()
    rep = lax.axis_index("rep")
    ins = [pltpu.make_async_copy(a, b, in_sem.at[i]) for i, (a, b) in enumerate(
        ((idx_h, idx), (pool_h, pool), (dense_h, dense), (cot_h, cot), (w_h, w)))]
    for cp in ins:
        cp.start()
    bar = pltpu.get_barrier_semaphore()
    with scope("bar"):
        for q in range(1, 32):
            pl.semaphore_signal(bar, 1, device_id=plane_peer(q), device_id_type=MESH)
        for d in range(1, 8):
            pl.semaphore_signal(bar, 1, device_id=z_peer(d), device_id_type=MESH)
    i0 = lax.broadcasted_iota(jnp.int32, (128, 128), 0)
    i1 = lax.broadcasted_iota(jnp.int32, (128, 128), 1)
    eye = (i0 == i1).astype(F32).astype(BF)
    one = jnp.float32(1)
    zero = jnp.float32(0)

    with scope("in0"):
        ins[0].wait()
    with scope("slots"):
        cols[...] = jnp.zeros_like(cols)
        keys, slots = [], []
        for l in range(2):
            row = idx[:, l, :]
            blk = row >> 6
            xx = ((row >> 10) & 1) * 2 + ((row >> 7) & 1)
            slot = ((xx ^ x) << 7) + ((((row >> 8) & 3) ^ y) << 5) + ((((row >> 6) & 1) ^ c) << 4)
            slot = slot + ((((row >> 11) - z) & 7) << 1)
            keys.append(((row & 63) + 1).astype(F32))
            slots.append(slot.astype(F32))
            cols[32 * l:32 * l + 26] = blk.astype(F32)
            sl[l] = blk.astype(F32)
        ct = cols[...].T
    with scope("rank"):
        sub = lax.broadcasted_iota(jnp.int32, (8, 128), 0)
        lane = lax.broadcasted_iota(jnp.int32, (8, 128), 1)
        for t in range(TABLES):
            b0 = jnp.broadcast_to(sl[0, t:t + 1], (8, 128))
            b1 = jnp.broadcast_to(sl[1, t:t + 1], (8, 128))
            n0 = jnp.zeros((8, 128), F32)
            n1 = n0
            for k in range(16):
                c0 = jnp.broadcast_to(ct[8 * k:8 * k + 8, t:t + 1], (8, 128))
                c1 = jnp.broadcast_to(ct[8 * k:8 * k + 8, 32 + t:33 + t], (8, 128))
                lt = jnp.where(sub + 8 * k < lane, one, zero)
                n0 = n0 + jnp.where(c0 == b0, lt, zero)
                n1 = n1 + jnp.where(c0 == b1, one, zero) + jnp.where(c1 == b1, lt, zero)
            cols[64 + t:65 + t] = jnp.sum(n0, axis=0, keepdims=True)
            cols[96 + t:97 + t] = jnp.sum(n1, axis=0, keepdims=True)
        for l in range(2):
            sl[l] = slots[l] + cols[64 + 32 * l:90 + 32 * l]

    def send_keys():
        for l in range(2):
            cols[32 * l:32 * l + 26] = sl[l]
            cols[64 + 32 * l:90 + 32 * l] = keys[l]
        ct = cols[...].T
        fl = lax.broadcasted_iota(jnp.int32, (8, 128), 1).astype(F32)
        lanes = [fl + jnp.float32(128 * b) for b in range(4)]
        keyt[...] = jnp.zeros_like(keyt)
        for t in range(TABLES):
            acc = [jnp.zeros((8, 128), F32)] * 4
            for k in range(16):
                col = [jnp.broadcast_to(ct[8 * k:8 * k + 8, 32 * j + t:32 * j + t + 1], (8, 128)) for j in range(4)]
                for b in range(4):
                    acc[b] = acc[b] + jnp.where(col[0] == lanes[b], col[2], zero) + jnp.where(col[1] == lanes[b], col[3], zero)
            for b in range(4):
                keyt[t:t + 1, 128 * b:128 * b + 128] = jnp.sum(acc[b], axis=0, keepdims=True)
        krow[...] = keyt[...].T.astype(BF)
        for q in range(1, 32):
            rcopy(krow.at[pl.ds(q * 16, 16)], krv.at[pl.ds(q * 16, 16)], k_send, s_recv.at[NC], plane_peer(q)).start()

    with scope("in1"):
        ins[1].wait()
        ins[2].wait()
    with scope("tr"):
        vt[0] = lax.dot_general(eye, dense[...], NT, preferred_element_type=F32)

        def tr(i, _):
            vt[i + 1] = lax.dot_general(eye, pool[i], NT, preferred_element_type=F32)
            return 0

        lax.fori_loop(0, TABLES, tr, 0, unroll=True)
    with scope("in3"):
        ins[3].wait()
        ins[4].wait()
    with scope("gt"):
        gt[0:479] = lax.dot_general(w[...], cot[...], NT, preferred_element_type=F32)
        gt[479:480] = jnp.zeros((1, 128), F32)
    with scope("barwait"):
        pl.semaphore_wait(bar, 38)

    def prow(a, b):
        hi = jnp.maximum(a, b)
        lo = jnp.minimum(a, b)
        return 128 + hi * (hi - 1) // 2 + lo

    def vg(i):
        acc = jnp.zeros((128, 128), F32)
        for j in range(27):
            p = jnp.where(i == j, 479, prow(i, jnp.int32(j)))
            acc = acc + gt[pl.ds(p, 1), :] * vt[j]
        return acc

    s512 = lax.broadcasted_iota(jnp.int32, (512, 128), 0).astype(F32)

    def compute(ch):
        t0, n = STARTS[ch], SIZES[ch]

        def table(t, _):
            v = vg(t + 1).astype(BF)
            p = jnp.where((s512 == sl[0, pl.ds(t, 1), :]) | (s512 == sl[1, pl.ds(t, 1), :]), one, zero)
            rows[t] = lax.dot_general(p.astype(BF), v, NT, preferred_element_type=F32).astype(BF)
            return 0

        lax.fori_loop(t0, t0 + n, table, 0, unroll=True)
        for q in range(1, 32):
            rcopy(rows.at[pl.ds(t0, n), pl.ds(q * 16, 16)], rv.at[pl.ds(t0, n), pl.ds(q * 16, 16)],
                  s_send, s_recv.at[ch], plane_peer(q)).start()

    def dense_part():
        d0 = vg(jnp.int32(0)) + gt[0:128]
        dgrad[...] = lax.dot_general(eye, d0.astype(BF), NT, preferred_element_type=F32).astype(BF)

    def core_copy():
        return rcopy(tp.at[1 - c], r0, t_send.at[0], t_recv.at[0], rep_peer(1))

    def top_part():
        g[0:128] = vt[0]
        g[479:480] = jnp.ones((1, 128), F32)

        def gram(i, _):
            va = vt[i]
            for d in range(1, 14):
                j = i + d
                j = jnp.where(j >= 27, j - 27, j)
                g[pl.ds(prow(i, j), 1), :] = jnp.sum(va * vt[j], axis=0, keepdims=True)
            return 0

        lax.fori_loop(0, 27, gram, 0)
        gb = g[...].astype(BF)
        for i in range(2):
            tp[i, 0:480] = jnp.dot(gb, cot[:, 512 * i:512 * i + 512], preferred_element_type=F32).astype(BF)
            tp[i, 480:512] = jnp.zeros((32, 512), BF)
        core_copy().start()

    def top_sum():
        core_copy().wait_recv()
        for k in range(8):
            at = pl.ds(pl.multiple_of((z + k) % 8 * 64, 64), 64)
            v = (tp[c, at].astype(F32) + r0[at].astype(F32)).astype(BF)
            for b in range(4):
                D[TABLES + b, k] = v[:, 128 * b:128 * b + 128]
        zcopy(0, 1, NC).start()
        zcopy(1, 1, NC).start()

    def spot(ref, xx, yy):
        return ref.at[yy, pl.ds(pl.multiple_of(xx * 16, 16), 16)]

    def p_target(q):
        return (x // 2 + q // 8) % 2 * 2 + (x + q // 4) % 2, (y // 2 + q // 2) % 2 * 2 + (y + q) % 2

    def p_share(q):
        return rcopy(spot(s1, *p_target(q)), r2.at[q - 1], t_send.at[2], t_recv.at[2], plane_peer(q * 2))

    def z_gather(d):
        return rcopy(pz, tb.at[c, x * 4 + y, z], t_send.at[3], t_recv.at[3], z_peer(d))

    def p_gather(q):
        reg = tb.at[c, x * 4 + y]
        return rcopy(reg, reg, t_send.at[4], t_recv.at[4], plane_peer(q * 2))

    def core_gather():
        return rcopy(tb.at[c], tb.at[c], t_send.at[5], t_recv.at[5], rep_peer(1))

    def top_share():
        z_wait(4, NC)
        for b in range(4):
            e = TABLES + b
            s1[b] = D[e, 0].astype(F32) + zr[0, 3, e].astype(F32) + zr[1, 3, e].astype(F32)
        for q in range(1, 16):
            p_share(q).start()

    def top_gather_z():
        wait_for(r2, t_recv.at[2])
        a = spot(s1, x, y)[...]
        for i in range(15):
            a = a + r2[i]
        pz[...] = a.astype(BF)
        tb[c, x * 4 + y, z] = a.astype(BF)
        for d in range(1, 8):
            z_gather(d).start()

    def top_gather_p():
        wait_for(tb.at[0, 0, pl.ds(0, 7)], t_recv.at[3])
        for q in range(1, 16):
            p_gather(q).start()

    def top_gather_c():
        wait_for(tb.at[0, pl.ds(0, 15)], t_recv.at[4])
        core_gather().start()

    def span(ch):
        return (STARTS[ch], SIZES[ch]) if ch < NC else (TABLES, 4)

    def zcopy(dirn, step, ch):
        t0, n = span(ch)
        rel = (5 - step) if dirn == 0 else (3 + step)
        lo, sz = (32 * dirn, 32) if step == 1 else (0, 64)
        return rcopy(D.at[pl.ds(t0, n), rel, pl.ds(lo, sz)], zr.at[dirn, step - 1, pl.ds(t0, n), pl.ds(lo, sz)],
                     z_send, z_recv.at[step - 1, ch], z_peer(1 if dirn == 0 else -1))

    def z_wait(step, ch):
        t0, n = span(ch)
        reg = zr.at[0, 0, pl.ds(t0, n)] if step == 1 else zr.at[pl.ds(0, 2), step - 1, pl.ds(t0, n)]
        wait_for(reg, z_recv.at[step - 1, ch])

    def acopy(i, ch):
        t0, n = STARTS[ch], SIZES[ch]
        reg = fin.at[pl.ds(t0, n), pl.ds(pl.multiple_of(rep * 64, 64), 64)]
        got = a_recv.at[0] if i == 2 and ch < RELAYED else a_recv.at[1]
        return rcopy(reg, reg, a_send, got, rep_peer(i))

    def fwd():
        reg = fin.at[pl.ds(0, TR), pl.ds(pl.multiple_of((rep + 2) % 4 * 64, 64), 64)]
        return rcopy(reg, reg, a_send, a_recv.at[1], rep_peer(1))

    rowi = lax.broadcasted_iota(jnp.int32, (512, 512), 0).astype(F32)

    def gather_keys():
        wait_for(krv.at[pl.ds(16, 496)], s_recv.at[NC])
        krv[0:16] = krow[0:16]
        kk = lax.dot_general(eye, krv[...], NT, preferred_element_type=F32)
        zz = (((lax.broadcasted_iota(jnp.int32, (128, 512), 1) >> 1) & 7) << 6).astype(F32)
        kt[...] = jnp.where(kk > 0.5, kk - 1 + zz, -1.0)

    def gather_rows(ch):
        t0, n = STARTS[ch], SIZES[ch]
        wait_for(rv.at[pl.ds(t0, n), pl.ds(16, 496)], s_recv.at[ch])
        rv[t0:t0 + n, 0:16] = rows[t0:t0 + n, 0:16]

        def acc(t, _):
            oh = jnp.where(rowi == kt[pl.ds(t, 1), :], one, zero).astype(BF)
            D[t] = jnp.dot(oh, rv[t], preferred_element_type=F32).astype(BF).reshape(8, 64, 128)
            return 0

        lax.fori_loop(t0, t0 + n, acc, 0, unroll=True)
        zcopy(0, 1, ch).start()
        zcopy(1, 1, ch).start()

    def zstep(s, ch):
        t0, n = span(ch)
        z_wait(s, ch)
        for dirn in (0, 1):
            rel = (4 - s) if dirn == 0 else (4 + s)
            lo, sz = (32 * dirn, 32) if s == 1 else (0, 64)
            for e in range(t0, t0 + n):
                D[e, rel, lo:lo + sz] = (D[e, rel, lo:lo + sz].astype(F32) + zr[dirn, s - 1, e, lo:lo + sz].astype(F32)).astype(BF)
            zcopy(dirn, s + 1, ch).start()

    def finish(ch):
        t0, n = STARTS[ch], SIZES[ch]
        z_wait(4, ch)
        for e in range(t0, t0 + n):
            v = D[e, 0].astype(F32) + zr[0, 3, e].astype(F32) + zr[1, 3, e].astype(F32)
            fin[e, pl.ds(pl.multiple_of(rep * 64, 64), 64)] = v.astype(BF)
        acopy(1, ch).start()
        acopy(2, ch).start()
        if ch >= RELAYED:
            acopy(3, ch).start()

    def named(name, f, *args):
        with scope(name):
            f(*args)

    chain = list(range(NC))
    chain.insert(TOP_AT + 1, NC)
    named("comp", compute, 0)
    named("comp", compute, 1)
    named("keys", send_keys)
    named("comp", compute, 2)
    named("top", top_part)
    made = AHEAD
    steps = len(chain) + 4 * LAG
    extra = {v: k for k, v in HOOKS.items()}
    acts = {"share": top_share, "gather_z": top_gather_z, "gather_p": top_gather_p, "gather_c": top_gather_c}
    for k in range(max(steps, max(extra) + 1)):
        if made < NC:
            named("comp", compute, made)
            made += 1
        elif made == NC:
            named("dense", dense_part)
            made += 1
        for s in (4, 3, 2, 1):
            i = k - LAG * s
            if 0 <= i < len(chain):
                ch = chain[i]
                if s < 4:
                    named("zs%d_%d" % (s, ch), zstep, s, ch)
                elif ch < NC:
                    named("fin%d" % ch, finish, ch)
        if k < len(chain):
            if chain[k] == NC:
                named("tsum", top_sum)
            else:
                if chain[k] == 0:
                    named("gkeys", gather_keys)
                named("gath%d" % chain[k], gather_rows, chain[k])
        if k in extra:
            named(extra[k], acts[extra[k]])
    with scope("fwd"):
        wait_for(fin.at[pl.ds(0, TR), pl.ds(0, 64)], a_recv.at[0])
        fwd().start()
    with scope("topw"):
        core_gather().wait_recv()
        for cc in range(2):
            for xx in range(4):
                for yy in range(4):
                    for zz in range(8):
                        r, q = zz * 64 + xx * 16, cc * 512 + yy * 128
                        if r < 464:
                            topo[r:r + 16, q:q + 128] = tb[cc, xx * 4 + yy, zz].astype(F32)
                        elif r == 464:
                            v = tb[cc, xx * 4 + yy, zz].astype(F32)
                            topo[r:r + 15, q:q + 128] = v[0:15]
                            bias[q // 128:q // 128 + 1] = v[15:16]
    with scope("tabw"):
        wait_for(zr.at[0, pl.ds(0, 2), pl.ds(0, REST // 2)], a_recv.at[1])
        tab[...] = fin[...].astype(F32)
    with scope("drain"):
        wait_for(fin.at[pl.ds(0, TABLES), pl.ds(0, 192)], a_send)
        wait_for(rows.at[pl.ds(0, TABLES), pl.ds(16, 496)], s_send)
        wait_for(D.at[pl.ds(0, TABLES + 4), pl.ds(0, 7)], z_send)
        wait_for(krow.at[pl.ds(16, 496)], k_send)
        core_copy().wait_send()
        wait_for(r2, t_send.at[2])
        wait_for(tb.at[0, 0, pl.ds(0, 7)], t_send.at[3])
        wait_for(tb.at[0, pl.ds(0, 15)], t_send.at[4])
        core_gather().wait_send()


def fused_call(dense, pool, w, cot, idx, cid=1, name="fused"):
    vm = pl.BlockSpec(memory_space=pltpu.VMEM)
    hbm = pl.BlockSpec(memory_space=pltpu.HBM)
    dma = pltpu.SemaphoreType.DMA
    V = pltpu.VMEM
    E = TABLES + 4
    return pl.pallas_call(
        kernel,
        out_shape=(
            jax.ShapeDtypeStruct((128, 128), BF),
            jax.ShapeDtypeStruct((479, 1024), F32),
            jax.ShapeDtypeStruct((8, 128), F32),
            jax.ShapeDtypeStruct((TABLES, 256, 128), F32),
        ),
        in_specs=[hbm] * 5,
        out_specs=(vm,) * 4,
        scratch_shapes=[
            V((128, 128), BF), V((TABLES, 128, 128), BF), V((479, 1024), BF), V((128, 1024), BF), V((TABLES, 2, 128), jnp.int32),
            V((27, 128, 128), F32), V((480, 128), F32), V((480, 128), F32), V((2, TABLES, 128), F32), V((128, 128), F32),
            V((128, 512), F32), V((512, 128), BF), V((512, 128), BF), V((128, 512), F32),
            V((TABLES, 512, 128), BF), V((TABLES, 512, 128), BF), V((E, 8, 64, 128), BF), V((2, 4, E, 64, 128), BF),
            V((TABLES, 256, 128), BF),
            V((2, 16, 8, 16, 128), BF), V((2, 512, 512), BF), V((512, 512), BF), V((4, 64, 128), F32), V((15, 16, 128), F32), V((16, 128), BF),
            dma((5,)), dma(()), dma(()), dma((NC + 1,)), dma(()), dma((4, NC + 1)), dma(()), dma((2,)), dma((6,)), dma((6,)),
        ],
        compiler_params=pltpu.CompilerParams(collective_id=cid, has_side_effects=True, vmem_limit_bytes=40 * 2**20),
        name=name,
    )(*[pltpu.with_memory_space_constraint(a, pltpu.HBM) for a in (dense, pool, w, cot, idx)])


def result_kernel(dgrad, topo, bias, tab, dgrad_o, topo_o, bias_o, tab_o, sem):
    pairs = [(tab.at[pl.ds(i, 2)], tab_o.at[pl.ds(i, 2)]) for i in range(0, TABLES, 2)]
    pairs += [(topo.at[pl.ds(i, 120)], topo_o.at[pl.ds(i, 120)]) for i in (0, 120, 240)]
    pairs += [(topo.at[pl.ds(360, 119)], topo_o.at[pl.ds(360, 119)]), (dgrad, dgrad_o), (bias, bias_o)]
    copies = [pltpu.make_async_copy(a, b, sem.at[i]) for i, (a, b) in enumerate(pairs)]
    for cp in copies:
        cp.start()
    for cp in copies:
        cp.wait()


def result_call(*arrays):
    vm = pl.BlockSpec(memory_space=pltpu.VMEM)
    hbm = pl.BlockSpec(memory_space=pltpu.HBM)
    return pl.pallas_call(
        result_kernel, out_shape=tuple(jax.ShapeDtypeStruct(a.shape, a.dtype) for a in arrays),
        in_specs=[vm] * 4, out_specs=(hbm,) * 4, scratch_shapes=[pltpu.SemaphoreType.DMA((19,))],
        compiler_params=pltpu.CompilerParams(vmem_limit_bytes=2**20), name="result")(*arrays)


def on_device(dense_out, pooled, top_weight, top_cotangent, indices):
    dgrad, top, bias, table = fused_call(
        dense_out, jnp.transpose(pooled, (1, 0, 2)), top_weight, top_cotangent, jnp.transpose(indices, (1, 2, 0)))
    dgrad, top, bias, table = result_call(dgrad, top, bias, table)
    return dgrad, top, bias.reshape(1024), table


def solution(mesh):
    both = P(("rep", "shard"))
    return jax.shard_map(
        on_device, mesh=mesh, in_specs=(both, both, P(), both, both),
        out_specs=(both, P(), P(), P(None, "shard", None)), check_vma=False)
```

```python
import contextlib

import jax
import jax.numpy as jnp
from jax import lax
from jax.experimental import pallas as pl
from jax.experimental.pallas import tpu as pltpu
from jax.sharding import PartitionSpec as P

F32 = jnp.float32
BF = jnp.bfloat16
NT = (((1,), (1,)), ((), ()))
MESH = pl.DeviceIdType.MESH
TABLES = 26
SIZES = (2,) * 13
NC = len(SIZES)
STARTS = tuple(sum(SIZES[:i]) for i in range(NC))
AHEAD = 3
GROUPS = (1,) * 13
CLOSE = {sum(GROUPS[:i + 1]) - 1: sum(GROUPS[:i]) for i in range(len(GROUPS))}
FLIP = 27
TOPK = -1


def lag_of(i, s):
    return LAG * s


LAG = 4
TOP_AT = -1
HOOKS = {"share": 8, "gather_z": 12, "gather_p": 15, "gather_c": 21}
RELAYED = NC - 1
TR = sum(SIZES[:RELAYED])
REST = 2 * TR + 3 * (TABLES - TR)
def scope(name):
    return contextlib.nullcontext()


def coords():
    r = lax.axis_index("rep")
    s = lax.axis_index("shard")
    return (s // 4) % 2 * 2 + r // 2, s % 4, s // 8, r % 2


def plane_peer(q):
    x, y, z, c = coords()
    xl = (x + q // 8) % 2
    xh = (x // 2 + q // 16) % 2
    yy = (y // 2 + q // 4) % 2 * 2 + (y + q // 2) % 2
    return (xl * 2 + (c + q) % 2, z * 8 + xh * 4 + yy)


def z_peer(d):
    return (lax.axis_index("rep"), (lax.axis_index("shard") + 8 * d + 64) % 64)


def rep_peer(i):
    r = lax.axis_index("rep")
    return ((r // 2 + i // 2) % 2 * 2 + (r + i) % 2, lax.axis_index("shard"))


def rcopy(src, dst, ss, rs, to):
    return pltpu.make_async_remote_copy(
        src_ref=src, dst_ref=dst, send_sem=ss, recv_sem=rs, device_id=to, device_id_type=MESH)


def wait_for(reg, sem):
    pltpu.make_async_copy(reg, reg, sem).wait()


def kernel(dense_h, pool_h, w_h, cot_h, idx_h, dgrad, topo, bias, tab,
           dense, pool, w, cot, idx, vt, g, gt, sl, blks, cols, keyt, krow, krv, kt,
           rows, rv, D, zr, fin, tb, tp, r0, s1, r2, pz,
           in_sem, s_send, k_send, s_recv, z_send, z_recv, a_send, a_recv, t_send, t_recv):
    x, y, z, c = coords()
    rep = lax.axis_index("rep")
    ins = [pltpu.make_async_copy(a, b, in_sem.at[i]) for i, (a, b) in enumerate(
        ((idx_h, idx), (pool_h, pool), (dense_h, dense), (cot_h, cot), (w_h, w)))]
    for cp in ins:
        cp.start()
    bar = pltpu.get_barrier_semaphore()
    with scope("bar"):
        for q in range(1, 32):
            pl.semaphore_signal(bar, 1, device_id=plane_peer(q), device_id_type=MESH)
        for d in range(1, 8):
            pl.semaphore_signal(bar, 1, device_id=z_peer(d), device_id_type=MESH)
    i0 = lax.broadcasted_iota(jnp.int32, (128, 128), 0)
    i1 = lax.broadcasted_iota(jnp.int32, (128, 128), 1)
    eye = (i0 == i1).astype(F32).astype(BF)
    one = jnp.float32(1)
    zero = jnp.float32(0)

    with scope("in0"):
        ins[0].wait()
    with scope("slots"):
        cols[...] = jnp.zeros_like(cols)
        keys, slots = [], []
        for l in range(2):
            row = idx[:, l, :]
            blk = row >> 6
            xx = ((row >> 10) & 1) * 2 + ((row >> 7) & 1)
            slot = ((xx ^ x) << 7) + ((((row >> 8) & 3) ^ y) << 5) + ((((row >> 6) & 1) ^ c) << 4)
            slot = slot + ((((row >> 11) - z) & 7) << 1)
            keys.append(((row & 63) + 1).astype(F32))
            slots.append(slot.astype(F32))
            cols[32 * l:32 * l + 26] = blk.astype(F32)
            blks[l] = blk.astype(F32)
        ct = cols[...].T
    base = slots

    def rank(tables):
        sub = lax.broadcasted_iota(jnp.int32, (8, 128), 0)
        lane = lax.broadcasted_iota(jnp.int32, (8, 128), 1)
        for t in tables:
            b0 = jnp.broadcast_to(blks[0, t:t + 1], (8, 128))
            b1 = jnp.broadcast_to(blks[1, t:t + 1], (8, 128))
            n0 = jnp.zeros((8, 128), F32)
            n1 = n0
            for k in range(16):
                c0 = jnp.broadcast_to(ct[8 * k:8 * k + 8, t:t + 1], (8, 128))
                c1 = jnp.broadcast_to(ct[8 * k:8 * k + 8, 32 + t:33 + t], (8, 128))
                lt = jnp.where(sub + 8 * k < lane, one, zero)
                n0 = n0 + jnp.where(c0 == b0, lt, zero)
                n1 = n1 + jnp.where(c0 == b1, one, zero) + jnp.where(c1 == b1, lt, zero)
            sl[0, t:t + 1] = base[0][t:t + 1] + jnp.sum(n0, axis=0, keepdims=True)
            sl[1, t:t + 1] = base[1][t:t + 1] + jnp.sum(n1, axis=0, keepdims=True)

    with scope("rank"):
        rank(range(SIZES[0]))

    def send_keys():
        for l in range(2):
            cols[32 * l:32 * l + 26] = sl[l]
            cols[64 + 32 * l:90 + 32 * l] = keys[l]
        ct = cols[...].T
        fl = lax.broadcasted_iota(jnp.int32, (8, 128), 1).astype(F32)
        lanes = [fl + jnp.float32(128 * b) for b in range(4)]
        keyt[...] = jnp.zeros_like(keyt)
        for t in range(TABLES):
            acc = [jnp.zeros((8, 128), F32)] * 4
            for k in range(16):
                col = [jnp.broadcast_to(ct[8 * k:8 * k + 8, 32 * j + t:32 * j + t + 1], (8, 128)) for j in range(4)]
                for b in range(4):
                    acc[b] = acc[b] + jnp.where(col[0] == lanes[b], col[2], zero) + jnp.where(col[1] == lanes[b], col[3], zero)
            for b in range(4):
                keyt[t:t + 1, 128 * b:128 * b + 128] = jnp.sum(acc[b], axis=0, keepdims=True)
        krow[...] = keyt[...].T.astype(BF)
        for q in range(1, 32):
            rcopy(krow.at[pl.ds(q * 16, 16)], krv.at[pl.ds(q * 16, 16)], k_send, s_recv.at[NC], plane_peer(q)).start()

    with scope("in1"):
        ins[1].wait()
        ins[2].wait()
    with scope("tr"):
        vt[0] = lax.dot_general(eye, dense[...], NT, preferred_element_type=F32)

        def tr(i, _):
            vt[i + 1] = lax.dot_general(eye, pool[i], NT, preferred_element_type=F32)
            return 0

        lax.fori_loop(0, TABLES, tr, 0, unroll=True)
    with scope("in3"):
        ins[3].wait()
        ins[4].wait()
    with scope("gt"):
        gt[0:479] = lax.dot_general(w[...], cot[...], NT, preferred_element_type=F32)
        gt[479:480] = jnp.zeros((1, 128), F32)
    with scope("barwait"):
        pl.semaphore_wait(bar, 38)

    def prow(a, b):
        hi = jnp.maximum(a, b)
        lo = jnp.minimum(a, b)
        return 128 + hi * (hi - 1) // 2 + lo

    def vg(i):
        acc = jnp.zeros((128, 128), F32)
        for j in range(27):
            p = jnp.where(i == j, 479, prow(i, jnp.int32(j)))
            acc = acc + gt[pl.ds(p, 1), :] * vt[j]
        return acc

    s512 = lax.broadcasted_iota(jnp.int32, (512, 128), 0).astype(F32)

    def compute(ch):
        t0, n = STARTS[ch], SIZES[ch]

        def table(t, _):
            v = vg(t + 1).astype(BF)
            p = jnp.where((s512 == sl[0, pl.ds(t, 1), :]) | (s512 == sl[1, pl.ds(t, 1), :]), one, zero)
            rows[t] = lax.dot_general(p.astype(BF), v, NT, preferred_element_type=F32).astype(BF)
            return 0

        lax.fori_loop(t0, t0 + n, table, 0, unroll=True)
        if ch in CLOSE:
            g0 = STARTS[CLOSE[ch]]
            n = t0 + n - g0
            for q in range(1, 32):
                rcopy(rows.at[pl.ds(g0, n), pl.ds(q * 16, 16)], rv.at[pl.ds(g0, n), pl.ds(q * 16, 16)],
                      s_send, s_recv.at[ch], plane_peer(q)).start()

    def dense_part():
        d0 = vg(jnp.int32(0)) + gt[0:128]
        dgrad[...] = lax.dot_general(eye, d0.astype(BF), NT, preferred_element_type=F32).astype(BF)

    def core_copy():
        return rcopy(tp.at[1 - c], r0, t_send.at[0], t_recv.at[0], rep_peer(1))

    def top_part():
        g[0:128] = vt[0]
        g[479:480] = jnp.ones((1, 128), F32)

        def gram(i, _):
            va = vt[i]
            for d in range(1, 14):
                j = i + d
                j = jnp.where(j >= 27, j - 27, j)
                g[pl.ds(prow(i, j), 1), :] = jnp.sum(va * vt[j], axis=0, keepdims=True)
            return 0

        lax.fori_loop(0, 27, gram, 0, unroll=3)
        gb = g[...].astype(BF)
        for i in range(2):
            tp[i, 0:480] = jnp.dot(gb, cot[:, 512 * i:512 * i + 512], preferred_element_type=F32).astype(BF)
            tp[i, 480:512] = jnp.zeros((32, 512), BF)
        core_copy().start()

    def top_sum():
        core_copy().wait_recv()
        for k in range(8):
            at = pl.ds(pl.multiple_of((z + k) % 8 * 64, 64), 64)
            v = (tp[c, at].astype(F32) + r0[at].astype(F32)).astype(BF)
            for b in range(4):
                D[TABLES + b, k] = v[:, 128 * b:128 * b + 128]
        zcopy(0, 1, NC).start()
        zcopy(1, 1, NC).start()

    def spot(ref, xx, yy):
        return ref.at[yy, pl.ds(pl.multiple_of(xx * 16, 16), 16)]

    def p_target(q):
        return (x // 2 + q // 8) % 2 * 2 + (x + q // 4) % 2, (y // 2 + q // 2) % 2 * 2 + (y + q) % 2

    def p_share(q):
        return rcopy(spot(s1, *p_target(q)), r2.at[q - 1], t_send.at[2], t_recv.at[2], plane_peer(q * 2))

    def z_gather(d):
        return rcopy(pz, tb.at[c, x * 4 + y, z], t_send.at[3], t_recv.at[3], z_peer(d))

    def p_gather(q):
        reg = tb.at[c, x * 4 + y]
        return rcopy(reg, reg, t_send.at[4], t_recv.at[4], plane_peer(q * 2))

    def core_gather():
        return rcopy(tb.at[c], tb.at[c], t_send.at[5], t_recv.at[5], rep_peer(1))

    def top_share():
        z_wait(4, NC)
        for b in range(4):
            e = TABLES + b
            s1[b] = D[e, 0].astype(F32) + zr[0, 3, e].astype(F32) + zr[1, 3, e].astype(F32)
        for q in range(1, 16):
            p_share(q).start()

    def top_gather_z():
        wait_for(r2, t_recv.at[2])
        a = spot(s1, x, y)[...]
        for i in range(15):
            a = a + r2[i]
        pz[...] = a.astype(BF)
        tb[c, x * 4 + y, z] = a.astype(BF)
        for d in range(1, 8):
            z_gather(d).start()

    def top_gather_p():
        wait_for(tb.at[0, 0, pl.ds(0, 7)], t_recv.at[3])
        for q in range(1, 16):
            p_gather(q).start()

    def top_gather_c():
        wait_for(tb.at[0, pl.ds(0, 15)], t_recv.at[4])
        core_gather().start()

    def span(ch):
        return (STARTS[ch], SIZES[ch]) if ch < NC else (TABLES, 4)

    def zcopy(dirn, step, ch):
        t0, n = span(ch)
        rel = (5 - step) if dirn == 0 else (3 + step)
        lo, sz = (32 * dirn, 32) if step == 1 else (0, 64)
        return rcopy(D.at[pl.ds(t0, n), rel, pl.ds(lo, sz)], zr.at[dirn, step - 1, pl.ds(t0, n), pl.ds(lo, sz)],
                     z_send, z_recv.at[step - 1, ch], z_peer(1 if dirn == 0 else -1))

    def z_wait(step, ch):
        t0, n = span(ch)
        reg = zr.at[0, 0, pl.ds(t0, n)] if step == 1 else zr.at[pl.ds(0, 2), step - 1, pl.ds(t0, n)]
        wait_for(reg, z_recv.at[step - 1, ch])

    def acopy(i, ch):
        t0, n = STARTS[ch], SIZES[ch]
        reg = fin.at[pl.ds(t0, n), pl.ds(pl.multiple_of(rep * 64, 64), 64)]
        got = a_recv.at[0] if i == 2 and ch < RELAYED else a_recv.at[1]
        return rcopy(reg, reg, a_send, got, rep_peer(i))

    def fwd():
        reg = fin.at[pl.ds(0, TR), pl.ds(pl.multiple_of((rep + 2) % 4 * 64, 64), 64)]
        return rcopy(reg, reg, a_send, a_recv.at[1], rep_peer(1))

    rowi = lax.broadcasted_iota(jnp.int32, (512, 512), 0).astype(F32)

    def gather_keys():
        wait_for(krv.at[pl.ds(16, 496)], s_recv.at[NC])
        krv[0:16] = krow[0:16]
        kk = lax.dot_general(eye, krv[...], NT, preferred_element_type=F32)
        zz = (((lax.broadcasted_iota(jnp.int32, (128, 512), 1) >> 1) & 7) << 6).astype(F32)
        kt[...] = jnp.where(kk > 0.5, kk - 1 + zz, -1.0)

    def gather_rows(ch):
        t0, n = STARTS[ch], SIZES[ch]
        for last, first in CLOSE.items():
            if first == ch:
                end = STARTS[last] + SIZES[last]
                wait_for(rv.at[pl.ds(t0, end - t0), pl.ds(16, 496)], s_recv.at[last])
        rv[t0:t0 + n, 0:16] = rows[t0:t0 + n, 0:16]

        def acc(t, _):
            oh = jnp.where(rowi == kt[pl.ds(t, 1), :], one, zero).astype(BF)
            D[t] = jnp.dot(oh, rv[t], preferred_element_type=F32).astype(BF).reshape(8, 64, 128)
            return 0

        lax.fori_loop(t0, t0 + n, acc, 0, unroll=True)
        zcopy(0, 1, ch).start()
        zcopy(1, 1, ch).start()

    def zstep(s, ch):
        t0, n = span(ch)
        z_wait(s, ch)
        for dirn in (0, 1):
            rel = (4 - s) if dirn == 0 else (4 + s)
            lo, sz = (32 * dirn, 32) if s == 1 else (0, 64)
            for e in range(t0, t0 + n):
                D[e, rel, lo:lo + sz] = (D[e, rel, lo:lo + sz].astype(F32) + zr[dirn, s - 1, e, lo:lo + sz].astype(F32)).astype(BF)
            zcopy(dirn, s + 1, ch).start()

    def finish(ch):
        t0, n = STARTS[ch], SIZES[ch]
        z_wait(4, ch)
        for e in range(t0, t0 + n):
            v = D[e, 0].astype(F32) + zr[0, 3, e].astype(F32) + zr[1, 3, e].astype(F32)
            fin[e, pl.ds(pl.multiple_of(rep * 64, 64), 64)] = v.astype(BF)
        acopy(1, ch).start()
        acopy(2, ch).start()
        if ch >= RELAYED:
            acopy(3, ch).start()

    def named(name, f, *args):
        with scope(name):
            f(*args)

    chain = list(range(NC))
    chain.insert(TOP_AT + 1, NC)
    named("comp", compute, 0)
    named("rank", rank, range(SIZES[0], TABLES))
    named("comp", compute, 1)
    named("keys", send_keys)
    named("comp", compute, 2)
    if TOPK < 0:
        named("top", top_part)
    made = AHEAD
    extra = {v: k for k, v in HOOKS.items()}
    acts = {"share": top_share, "gather_z": top_gather_z, "gather_p": top_gather_p, "gather_c": top_gather_c}
    halves = {}
    for i, ch in enumerate(chain):
        for s in (1, 2, 3, 4):
            halves.setdefault(2 * i + lag_of(i, s), []).append((i, s, ch))
    n = max(max(halves), 2 * max(extra) + 1) + 1
    for h in range(n):
        k = h // 2
        if h % 2 == 0:
            if made < NC:
                named("comp", compute, made)
                made += 1
            elif made == NC:
                named("dense", dense_part)
                made += 1
        for i, s, ch in sorted(halves.get(h, []), reverse=h >= FLIP):
            if s < 4:
                named("zs%d_%d" % (s, ch), zstep, s, ch)
            elif ch < NC:
                named("fin%d" % ch, finish, ch)
        if h % 2 == 0 and k < len(chain):
            if chain[k] == NC:
                named("tsum", top_sum)
            else:
                if chain[k] == 0:
                    named("gkeys", gather_keys)
                named("gath%d" % chain[k], gather_rows, chain[k])
        if h == 2 * TOPK:
            named("top", top_part)
        if h % 2 == 1 and k in extra:
            named(extra[k], acts[extra[k]])
    with scope("fwd"):
        wait_for(fin.at[pl.ds(0, TR), pl.ds(0, 64)], a_recv.at[0])
        fwd().start()
    with scope("topw"):
        core_gather().wait_recv()
        for cc in range(2):
            for xx in range(4):
                for yy in range(4):
                    for zz in range(8):
                        r, q = zz * 64 + xx * 16, cc * 512 + yy * 128
                        if r < 464:
                            topo[r:r + 16, q:q + 128] = tb[cc, xx * 4 + yy, zz].astype(F32)
                        elif r == 464:
                            v = tb[cc, xx * 4 + yy, zz].astype(F32)
                            topo[r:r + 15, q:q + 128] = v[0:15]
                            bias[q // 128:q // 128 + 1] = v[15:16]
    with scope("tabw"):
        wait_for(zr.at[0, pl.ds(0, 2), pl.ds(0, REST // 2)], a_recv.at[1])
        tab[...] = fin[...].astype(F32)
    with scope("drain"):
        wait_for(fin.at[pl.ds(0, TABLES), pl.ds(0, 192)], a_send)
        wait_for(rows.at[pl.ds(0, TABLES), pl.ds(16, 496)], s_send)
        wait_for(D.at[pl.ds(0, TABLES + 4), pl.ds(0, 7)], z_send)
        wait_for(krow.at[pl.ds(16, 496)], k_send)
        core_copy().wait_send()
        wait_for(r2, t_send.at[2])
        wait_for(tb.at[0, 0, pl.ds(0, 7)], t_send.at[3])
        wait_for(tb.at[0, pl.ds(0, 15)], t_send.at[4])
        core_gather().wait_send()


def fused_call(dense, pool, w, cot, idx, cid=1, name="fused"):
    vm = pl.BlockSpec(memory_space=pltpu.VMEM)
    hbm = pl.BlockSpec(memory_space=pltpu.HBM)
    dma = pltpu.SemaphoreType.DMA
    V = pltpu.VMEM
    E = TABLES + 4
    return pl.pallas_call(
        kernel,
        out_shape=(
            jax.ShapeDtypeStruct((128, 128), BF),
            jax.ShapeDtypeStruct((479, 1024), F32),
            jax.ShapeDtypeStruct((8, 128), F32),
            jax.ShapeDtypeStruct((TABLES, 256, 128), F32),
        ),
        in_specs=[hbm] * 5,
        out_specs=(vm,) * 4,
        scratch_shapes=[
            V((128, 128), BF), V((TABLES, 128, 128), BF), V((479, 1024), BF), V((128, 1024), BF), V((TABLES, 2, 128), jnp.int32),
            V((27, 128, 128), F32), V((480, 128), F32), V((480, 128), F32), V((2, TABLES, 128), F32), V((2, TABLES, 128), F32), V((128, 128), F32),
            V((128, 512), F32), V((512, 128), BF), V((512, 128), BF), V((128, 512), F32),
            V((TABLES, 512, 128), BF), V((TABLES, 512, 128), BF), V((E, 8, 64, 128), BF), V((2, 4, E, 64, 128), BF),
            V((TABLES, 256, 128), BF),
            V((2, 16, 8, 16, 128), BF), V((2, 512, 512), BF), V((512, 512), BF), V((4, 64, 128), F32), V((15, 16, 128), F32), V((16, 128), BF),
            dma((5,)), dma(()), dma(()), dma((NC + 1,)), dma(()), dma((4, NC + 1)), dma(()), dma((2,)), dma((6,)), dma((6,)),
        ],
        compiler_params=pltpu.CompilerParams(collective_id=cid, has_side_effects=True, vmem_limit_bytes=40 * 2**20),
        name=name,
    )(*[pltpu.with_memory_space_constraint(a, pltpu.HBM) for a in (dense, pool, w, cot, idx)])


def result_kernel(dgrad, topo, bias, tab, dgrad_o, topo_o, bias_o, tab_o, sem):
    pairs = [(tab.at[pl.ds(i, 2)], tab_o.at[pl.ds(i, 2)]) for i in range(0, TABLES, 2)]
    pairs += [(topo.at[pl.ds(i, 120)], topo_o.at[pl.ds(i, 120)]) for i in (0, 120, 240)]
    pairs += [(topo.at[pl.ds(360, 119)], topo_o.at[pl.ds(360, 119)]), (dgrad, dgrad_o), (bias, bias_o)]
    copies = [pltpu.make_async_copy(a, b, sem.at[i]) for i, (a, b) in enumerate(pairs)]
    for cp in copies:
        cp.start()
    for cp in copies:
        cp.wait()


def result_call(*arrays):
    vm = pl.BlockSpec(memory_space=pltpu.VMEM)
    hbm = pl.BlockSpec(memory_space=pltpu.HBM)
    return pl.pallas_call(
        result_kernel, out_shape=tuple(jax.ShapeDtypeStruct(a.shape, a.dtype) for a in arrays),
        in_specs=[vm] * 4, out_specs=(hbm,) * 4, scratch_shapes=[pltpu.SemaphoreType.DMA((19,))],
        compiler_params=pltpu.CompilerParams(vmem_limit_bytes=2**20), name="result")(*arrays)


def on_device(dense_out, pooled, top_weight, top_cotangent, indices):
    dgrad, top, bias, table = fused_call(
        dense_out, jnp.transpose(pooled, (1, 0, 2)), top_weight, top_cotangent, jnp.transpose(indices, (1, 2, 0)))
    dgrad, top, bias, table = result_call(dgrad, top, bias, table)
    return dgrad, top, bias.reshape(1024), table


def solution(mesh):
    both = P(("rep", "shard"))
    return jax.shard_map(
        on_device, mesh=mesh, in_specs=(both, both, P(), both, both),
        out_specs=(both, P(), P(), P(None, "shard", None)), check_vma=False)
```

```python
import contextlib

import jax
import jax.numpy as jnp
from jax import lax
from jax.experimental import pallas as pl
from jax.experimental.pallas import tpu as pltpu
from jax.sharding import PartitionSpec as P

F32 = jnp.float32
BF = jnp.bfloat16
NT = (((1,), (1,)), ((), ()))
MESH = pl.DeviceIdType.MESH
TABLES = 26
SIZES = (2,) * 13
NC = len(SIZES)
STARTS = tuple(sum(SIZES[:i]) for i in range(NC))
AHEAD = 3
GROUPS = (1,) * 13
CLOSE = {sum(GROUPS[:i + 1]) - 1: sum(GROUPS[:i]) for i in range(len(GROUPS))}
FLIP = 27
TOPK = -1


def lag_of(i, s):
    return LAG * s


LAG = 4
TOP_AT = -1
HOOKS = {"share": 8, "gather_z": 12, "gather_p": 14, "gather_c": 21}
RELAYED = NC - 1
TR = sum(SIZES[:RELAYED])
REST = 2 * TR + 3 * (TABLES - TR)
def scope(name):
    return contextlib.nullcontext()


def coords():
    r = lax.axis_index("rep")
    s = lax.axis_index("shard")
    return (s // 4) % 2 * 2 + r // 2, s % 4, s // 8, r % 2


def plane_peer(q):
    x, y, z, c = coords()
    xl = (x + q // 8) % 2
    xh = (x // 2 + q // 16) % 2
    yy = (y // 2 + q // 4) % 2 * 2 + (y + q // 2) % 2
    return (xl * 2 + (c + q) % 2, z * 8 + xh * 4 + yy)


def z_peer(d):
    return (lax.axis_index("rep"), (lax.axis_index("shard") + 8 * d + 64) % 64)


def rep_peer(i):
    r = lax.axis_index("rep")
    return ((r // 2 + i // 2) % 2 * 2 + (r + i) % 2, lax.axis_index("shard"))


def rcopy(src, dst, ss, rs, to):
    return pltpu.make_async_remote_copy(
        src_ref=src, dst_ref=dst, send_sem=ss, recv_sem=rs, device_id=to, device_id_type=MESH)


def wait_for(reg, sem):
    pltpu.make_async_copy(reg, reg, sem).wait()


def kernel(dense_h, pool_h, w_h, cot_h, idx_h, dgrad, topo, bias, tab,
           dense, pool, w, cot, idx, vt, g, gt, sl, blks, cols, keyt, krow, krv, kt,
           rows, rv, D, zr, fin, tb, tp, r0, s1, r2, pz,
           in_sem, s_send, k_send, s_recv, z_send, z_recv, a_send, a_recv, t_send, t_recv):
    x, y, z, c = coords()
    rep = lax.axis_index("rep")
    ins = [pltpu.make_async_copy(a, b, in_sem.at[i]) for i, (a, b) in enumerate(
        ((idx_h, idx), (pool_h, pool), (dense_h, dense), (cot_h, cot), (w_h, w)))]
    for cp in ins:
        cp.start()
    bar = pltpu.get_barrier_semaphore()
    with scope("bar"):
        for q in range(1, 32):
            pl.semaphore_signal(bar, 1, device_id=plane_peer(q), device_id_type=MESH)
        for d in range(1, 8):
            pl.semaphore_signal(bar, 1, device_id=z_peer(d), device_id_type=MESH)
    i0 = lax.broadcasted_iota(jnp.int32, (128, 128), 0)
    i1 = lax.broadcasted_iota(jnp.int32, (128, 128), 1)
    eye = (i0 == i1).astype(F32).astype(BF)
    one = jnp.float32(1)
    zero = jnp.float32(0)

    with scope("in0"):
        ins[0].wait()
    with scope("slots"):
        cols[...] = jnp.zeros_like(cols)
        keys, slots = [], []
        for l in range(2):
            row = idx[:, l, :]
            blk = row >> 6
            xx = ((row >> 10) & 1) * 2 + ((row >> 7) & 1)
            slot = ((xx ^ x) << 7) + ((((row >> 8) & 3) ^ y) << 5) + ((((row >> 6) & 1) ^ c) << 4)
            slot = slot + ((((row >> 11) - z) & 7) << 1)
            keys.append(((row & 63) + 1).astype(F32))
            slots.append(slot.astype(F32))
            cols[32 * l:32 * l + 26] = blk.astype(F32)
            blks[l] = blk.astype(F32)
        ct = cols[...].T
    base = slots

    def rank(tables):
        sub = lax.broadcasted_iota(jnp.int32, (8, 128), 0)
        lane = lax.broadcasted_iota(jnp.int32, (8, 128), 1)
        for t in tables:
            b0 = jnp.broadcast_to(blks[0, t:t + 1], (8, 128))
            b1 = jnp.broadcast_to(blks[1, t:t + 1], (8, 128))
            n0 = jnp.zeros((8, 128), F32)
            n1 = n0
            for k in range(16):
                c0 = jnp.broadcast_to(ct[8 * k:8 * k + 8, t:t + 1], (8, 128))
                c1 = jnp.broadcast_to(ct[8 * k:8 * k + 8, 32 + t:33 + t], (8, 128))
                lt = jnp.where(sub + 8 * k < lane, one, zero)
                n0 = n0 + jnp.where(c0 == b0, lt, zero)
                n1 = n1 + jnp.where(c0 == b1, one, zero) + jnp.where(c1 == b1, lt, zero)
            sl[0, t:t + 1] = base[0][t:t + 1] + jnp.sum(n0, axis=0, keepdims=True)
            sl[1, t:t + 1] = base[1][t:t + 1] + jnp.sum(n1, axis=0, keepdims=True)

    with scope("rank"):
        rank(range(SIZES[0]))

    def send_keys():
        for l in range(2):
            cols[32 * l:32 * l + 26] = sl[l]
            cols[64 + 32 * l:90 + 32 * l] = keys[l]
        ct = cols[...].T
        fl = lax.broadcasted_iota(jnp.int32, (8, 128), 1).astype(F32)
        lanes = [fl + jnp.float32(128 * b) for b in range(4)]
        keyt[...] = jnp.zeros_like(keyt)
        for t in range(TABLES):
            acc = [jnp.zeros((8, 128), F32)] * 4
            for k in range(16):
                col = [jnp.broadcast_to(ct[8 * k:8 * k + 8, 32 * j + t:32 * j + t + 1], (8, 128)) for j in range(4)]
                for b in range(4):
                    acc[b] = acc[b] + jnp.where(col[0] == lanes[b], col[2], zero) + jnp.where(col[1] == lanes[b], col[3], zero)
            for b in range(4):
                keyt[t:t + 1, 128 * b:128 * b + 128] = jnp.sum(acc[b], axis=0, keepdims=True)
        krow[...] = keyt[...].T.astype(BF)
        for q in range(1, 32):
            rcopy(krow.at[pl.ds(q * 16, 16)], krv.at[pl.ds(q * 16, 16)], k_send, s_recv.at[NC], plane_peer(q)).start()

    with scope("in1"):
        ins[1].wait()
        ins[2].wait()
    with scope("tr"):
        vt[0] = lax.dot_general(eye, dense[...], NT, preferred_element_type=F32)

        def tr(i, _):
            vt[i + 1] = lax.dot_general(eye, pool[i], NT, preferred_element_type=F32)
            return 0

        lax.fori_loop(0, TABLES, tr, 0, unroll=True)
    with scope("in3"):
        ins[3].wait()
        ins[4].wait()
    with scope("gt"):
        gt[0:479] = lax.dot_general(w[...], cot[...], NT, preferred_element_type=F32)
        gt[479:480] = jnp.zeros((1, 128), F32)
    with scope("barwait"):
        pl.semaphore_wait(bar, 38)

    def prow(a, b):
        hi = jnp.maximum(a, b)
        lo = jnp.minimum(a, b)
        return 128 + hi * (hi - 1) // 2 + lo

    def vg(i):
        acc = jnp.zeros((128, 128), F32)
        for j in range(27):
            p = jnp.where(i == j, 479, prow(i, jnp.int32(j)))
            acc = acc + gt[pl.ds(p, 1), :] * vt[j]
        return acc

    s512 = lax.broadcasted_iota(jnp.int32, (512, 128), 0).astype(F32)

    def compute(ch):
        t0, n = STARTS[ch], SIZES[ch]

        def table(t, _):
            v = vg(t + 1).astype(BF)
            p = jnp.where((s512 == sl[0, pl.ds(t, 1), :]) | (s512 == sl[1, pl.ds(t, 1), :]), one, zero)
            rows[t] = lax.dot_general(p.astype(BF), v, NT, preferred_element_type=F32).astype(BF)
            return 0

        lax.fori_loop(t0, t0 + n, table, 0, unroll=True)
        if ch in CLOSE:
            g0 = STARTS[CLOSE[ch]]
            n = t0 + n - g0
            for q in range(1, 32):
                rcopy(rows.at[pl.ds(g0, n), pl.ds(q * 16, 16)], rv.at[pl.ds(g0, n), pl.ds(q * 16, 16)],
                      s_send, s_recv.at[ch], plane_peer(q)).start()

    def dense_part():
        d0 = vg(jnp.int32(0)) + gt[0:128]
        dgrad[...] = lax.dot_general(eye, d0.astype(BF), NT, preferred_element_type=F32).astype(BF)

    def core_copy():
        return rcopy(tp.at[1 - c], r0, t_send.at[0], t_recv.at[0], rep_peer(1))

    def top_part():
        g[0:128] = vt[0]
        g[479:480] = jnp.ones((1, 128), F32)

        def gram(i, _):
            va = vt[i]
            for d in range(1, 14):
                j = i + d
                j = jnp.where(j >= 27, j - 27, j)
                g[pl.ds(prow(i, j), 1), :] = jnp.sum(va * vt[j], axis=0, keepdims=True)
            return 0

        lax.fori_loop(0, 27, gram, 0, unroll=3)
        gb = g[...].astype(BF)
        for i in range(2):
            tp[i, 0:480] = jnp.dot(gb, cot[:, 512 * i:512 * i + 512], preferred_element_type=F32).astype(BF)
            tp[i, 480:512] = jnp.zeros((32, 512), BF)
        core_copy().start()

    def top_sum():
        core_copy().wait_recv()
        for k in range(8):
            at = pl.ds(pl.multiple_of((z + k) % 8 * 64, 64), 64)
            v = (tp[c, at].astype(F32) + r0[at].astype(F32)).astype(BF)
            for b in range(4):
                D[TABLES + b, k] = v[:, 128 * b:128 * b + 128]
        zcopy(0, 1, NC).start()
        zcopy(1, 1, NC).start()

    def spot(ref, xx, yy):
        return ref.at[yy, pl.ds(pl.multiple_of(xx * 16, 16), 16)]

    def p_target(q):
        return (x // 2 + q // 8) % 2 * 2 + (x + q // 4) % 2, (y // 2 + q // 2) % 2 * 2 + (y + q) % 2

    def p_share(q):
        return rcopy(spot(s1, *p_target(q)), r2.at[q - 1], t_send.at[2], t_recv.at[2], plane_peer(q * 2))

    def z_gather(d):
        return rcopy(pz, tb.at[c, x * 4 + y, z], t_send.at[3], t_recv.at[3], z_peer(d))

    def p_gather(q):
        reg = tb.at[c, x * 4 + y]
        return rcopy(reg, reg, t_send.at[4], t_recv.at[4], plane_peer(q * 2))

    def core_gather():
        return rcopy(tb.at[c], tb.at[c], t_send.at[5], t_recv.at[5], rep_peer(1))

    def top_share():
        z_wait(4, NC)
        for b in range(4):
            e = TABLES + b
            s1[b] = D[e, 0].astype(F32) + zr[0, 3, e].astype(F32) + zr[1, 3, e].astype(F32)
        for q in range(1, 16):
            p_share(q).start()

    def top_gather_z():
        wait_for(r2, t_recv.at[2])
        a = spot(s1, x, y)[...]
        for i in range(15):
            a = a + r2[i]
        pz[...] = a.astype(BF)
        tb[c, x * 4 + y, z] = a.astype(BF)
        for d in range(1, 8):
            z_gather(d).start()

    def top_gather_p():
        wait_for(tb.at[0, 0, pl.ds(0, 7)], t_recv.at[3])
        for q in range(1, 16):
            p_gather(q).start()

    def top_gather_c():
        wait_for(tb.at[0, pl.ds(0, 15)], t_recv.at[4])
        core_gather().start()

    def span(ch):
        return (STARTS[ch], SIZES[ch]) if ch < NC else (TABLES, 4)

    def zcopy(dirn, step, ch):
        t0, n = span(ch)
        rel = (5 - step) if dirn == 0 else (3 + step)
        lo, sz = (32 * dirn, 32) if step == 1 else (0, 64)
        return rcopy(D.at[pl.ds(t0, n), rel, pl.ds(lo, sz)], zr.at[dirn, step - 1, pl.ds(t0, n), pl.ds(lo, sz)],
                     z_send, z_recv.at[step - 1, ch], z_peer(1 if dirn == 0 else -1))

    def z_wait(step, ch):
        t0, n = span(ch)
        reg = zr.at[0, 0, pl.ds(t0, n)] if step == 1 else zr.at[pl.ds(0, 2), step - 1, pl.ds(t0, n)]
        wait_for(reg, z_recv.at[step - 1, ch])

    def acopy(i, ch):
        t0, n = STARTS[ch], SIZES[ch]
        reg = fin.at[pl.ds(t0, n), pl.ds(pl.multiple_of(rep * 64, 64), 64)]
        got = a_recv.at[0] if i == 2 and ch < RELAYED else a_recv.at[1]
        return rcopy(reg, reg, a_send, got, rep_peer(i))

    def fwd():
        reg = fin.at[pl.ds(0, TR), pl.ds(pl.multiple_of((rep + 2) % 4 * 64, 64), 64)]
        return rcopy(reg, reg, a_send, a_recv.at[1], rep_peer(1))

    rowi = lax.broadcasted_iota(jnp.int32, (512, 512), 0).astype(F32)

    def gather_keys():
        wait_for(krv.at[pl.ds(16, 496)], s_recv.at[NC])
        krv[0:16] = krow[0:16]
        kk = lax.dot_general(eye, krv[...], NT, preferred_element_type=F32)
        zz = (((lax.broadcasted_iota(jnp.int32, (128, 512), 1) >> 1) & 7) << 6).astype(F32)
        kt[...] = jnp.where(kk > 0.5, kk - 1 + zz, -1.0)

    def gather_rows(ch):
        t0, n = STARTS[ch], SIZES[ch]
        for last, first in CLOSE.items():
            if first == ch:
                end = STARTS[last] + SIZES[last]
                wait_for(rv.at[pl.ds(t0, end - t0), pl.ds(16, 496)], s_recv.at[last])
        rv[t0:t0 + n, 0:16] = rows[t0:t0 + n, 0:16]

        def acc(t, _):
            oh = jnp.where(rowi == kt[pl.ds(t, 1), :], one, zero).astype(BF)
            D[t] = jnp.dot(oh, rv[t], preferred_element_type=F32).astype(BF).reshape(8, 64, 128)
            return 0

        lax.fori_loop(t0, t0 + n, acc, 0, unroll=True)
        zcopy(0, 1, ch).start()
        zcopy(1, 1, ch).start()

    def zstep(s, ch):
        t0, n = span(ch)
        z_wait(s, ch)
        for dirn in (0, 1):
            rel = (4 - s) if dirn == 0 else (4 + s)
            lo, sz = (32 * dirn, 32) if s == 1 else (0, 64)
            for e in range(t0, t0 + n):
                D[e, rel, lo:lo + sz] = (D[e, rel, lo:lo + sz].astype(F32) + zr[dirn, s - 1, e, lo:lo + sz].astype(F32)).astype(BF)
            zcopy(dirn, s + 1, ch).start()

    def finish(ch):
        t0, n = STARTS[ch], SIZES[ch]
        z_wait(4, ch)
        for e in range(t0, t0 + n):
            v = D[e, 0].astype(F32) + zr[0, 3, e].astype(F32) + zr[1, 3, e].astype(F32)
            fin[e, pl.ds(pl.multiple_of(rep * 64, 64), 64)] = v.astype(BF)
        acopy(1, ch).start()
        acopy(2, ch).start()
        if ch >= RELAYED:
            acopy(3, ch).start()

    def named(name, f, *args):
        with scope(name):
            f(*args)

    chain = list(range(NC))
    chain.insert(TOP_AT + 1, NC)
    named("comp", compute, 0)
    named("rank", rank, range(SIZES[0], TABLES))
    named("comp", compute, 1)
    named("keys", send_keys)
    named("comp", compute, 2)
    if TOPK < 0:
        named("top", top_part)
    made = AHEAD
    extra = {v: k for k, v in HOOKS.items()}
    acts = {"share": top_share, "gather_z": top_gather_z, "gather_p": top_gather_p, "gather_c": top_gather_c}
    halves = {}
    for i, ch in enumerate(chain):
        for s in (1, 2, 3, 4):
            halves.setdefault(2 * i + lag_of(i, s), []).append((i, s, ch))
    n = max(max(halves), 2 * max(extra) + 1) + 1
    for h in range(n):
        k = h // 2
        if h % 2 == 0:
            if made < NC:
                named("comp", compute, made)
                made += 1
            elif made == NC:
                named("dense", dense_part)
                made += 1
        for i, s, ch in sorted(halves.get(h, []), reverse=h >= FLIP):
            if s < 4:
                named("zs%d_%d" % (s, ch), zstep, s, ch)
            elif ch < NC:
                named("fin%d" % ch, finish, ch)
        if h % 2 == 0 and k < len(chain):
            if chain[k] == NC:
                named("tsum", top_sum)
            else:
                if chain[k] == 0:
                    named("gkeys", gather_keys)
                named("gath%d" % chain[k], gather_rows, chain[k])
        if h == 2 * TOPK:
            named("top", top_part)
        if h % 2 == 1 and k in extra:
            named(extra[k], acts[extra[k]])
    with scope("fwd"):
        wait_for(fin.at[pl.ds(0, TR), pl.ds(0, 64)], a_recv.at[0])
        fwd().start()
    with scope("topw"):
        core_gather().wait_recv()
        for cc in range(2):
            for xx in range(4):
                for yy in range(4):
                    for zz in range(8):
                        r, q = zz * 64 + xx * 16, cc * 512 + yy * 128
                        if r < 464:
                            topo[r:r + 16, q:q + 128] = tb[cc, xx * 4 + yy, zz].astype(F32)
                        elif r == 464:
                            v = tb[cc, xx * 4 + yy, zz].astype(F32)
                            topo[r:r + 15, q:q + 128] = v[0:15]
                            bias[q // 128:q // 128 + 1] = v[15:16]
    with scope("tabw"):
        wait_for(zr.at[0, pl.ds(0, 2), pl.ds(0, REST // 2)], a_recv.at[1])
        tab[...] = fin[...].astype(F32)
    with scope("drain"):
        wait_for(fin.at[pl.ds(0, TABLES), pl.ds(0, 192)], a_send)
        wait_for(rows.at[pl.ds(0, TABLES), pl.ds(16, 496)], s_send)
        wait_for(D.at[pl.ds(0, TABLES + 4), pl.ds(0, 7)], z_send)
        wait_for(krow.at[pl.ds(16, 496)], k_send)
        core_copy().wait_send()
        wait_for(r2, t_send.at[2])
        wait_for(tb.at[0, 0, pl.ds(0, 7)], t_send.at[3])
        wait_for(tb.at[0, pl.ds(0, 15)], t_send.at[4])
        core_gather().wait_send()


def fused_call(dense, pool, w, cot, idx, cid=1, name="fused"):
    vm = pl.BlockSpec(memory_space=pltpu.VMEM)
    hbm = pl.BlockSpec(memory_space=pltpu.HBM)
    dma = pltpu.SemaphoreType.DMA
    V = pltpu.VMEM
    E = TABLES + 4
    return pl.pallas_call(
        kernel,
        out_shape=(
            jax.ShapeDtypeStruct((128, 128), BF),
            jax.ShapeDtypeStruct((479, 1024), F32),
            jax.ShapeDtypeStruct((8, 128), F32),
            jax.ShapeDtypeStruct((TABLES, 256, 128), F32),
        ),
        in_specs=[hbm] * 5,
        out_specs=(vm,) * 4,
        scratch_shapes=[
            V((128, 128), BF), V((TABLES, 128, 128), BF), V((479, 1024), BF), V((128, 1024), BF), V((TABLES, 2, 128), jnp.int32),
            V((27, 128, 128), F32), V((480, 128), F32), V((480, 128), F32), V((2, TABLES, 128), F32), V((2, TABLES, 128), F32), V((128, 128), F32),
            V((128, 512), F32), V((512, 128), BF), V((512, 128), BF), V((128, 512), F32),
            V((TABLES, 512, 128), BF), V((TABLES, 512, 128), BF), V((E, 8, 64, 128), BF), V((2, 4, E, 64, 128), BF),
            V((TABLES, 256, 128), BF),
            V((2, 16, 8, 16, 128), BF), V((2, 512, 512), BF), V((512, 512), BF), V((4, 64, 128), F32), V((15, 16, 128), F32), V((16, 128), BF),
            dma((5,)), dma(()), dma(()), dma((NC + 1,)), dma(()), dma((4, NC + 1)), dma(()), dma((2,)), dma((6,)), dma((6,)),
        ],
        compiler_params=pltpu.CompilerParams(collective_id=cid, has_side_effects=True, vmem_limit_bytes=40 * 2**20),
        name=name,
    )(*[pltpu.with_memory_space_constraint(a, pltpu.HBM) for a in (dense, pool, w, cot, idx)])


def result_kernel(dgrad, topo, bias, tab, dgrad_o, topo_o, bias_o, tab_o, sem):
    pairs = [(tab.at[pl.ds(i, 2)], tab_o.at[pl.ds(i, 2)]) for i in range(0, TABLES, 2)]
    pairs += [(topo.at[pl.ds(i, 120)], topo_o.at[pl.ds(i, 120)]) for i in (0, 120, 240)]
    pairs += [(topo.at[pl.ds(360, 119)], topo_o.at[pl.ds(360, 119)]), (dgrad, dgrad_o), (bias, bias_o)]
    copies = [pltpu.make_async_copy(a, b, sem.at[i]) for i, (a, b) in enumerate(pairs)]
    for cp in copies:
        cp.start()
    for cp in copies:
        cp.wait()


def result_call(*arrays):
    vm = pl.BlockSpec(memory_space=pltpu.VMEM)
    hbm = pl.BlockSpec(memory_space=pltpu.HBM)
    return pl.pallas_call(
        result_kernel, out_shape=tuple(jax.ShapeDtypeStruct(a.shape, a.dtype) for a in arrays),
        in_specs=[vm] * 4, out_specs=(hbm,) * 4, scratch_shapes=[pltpu.SemaphoreType.DMA((19,))],
        compiler_params=pltpu.CompilerParams(vmem_limit_bytes=2**20), name="result")(*arrays)


def on_device(dense_out, pooled, top_weight, top_cotangent, indices):
    dgrad, top, bias, table = fused_call(
        dense_out, jnp.transpose(pooled, (1, 0, 2)), top_weight, top_cotangent, jnp.transpose(indices, (1, 2, 0)))
    dgrad, top, bias, table = result_call(dgrad, top, bias, table)
    return dgrad, top, bias.reshape(1024), table


def solution(mesh):
    both = P(("rep", "shard"))
    return jax.shard_map(
        on_device, mesh=mesh, in_specs=(both, both, P(), both, both),
        out_specs=(both, P(), P(), P(None, "shard", None)), check_vma=False)
```

```python
import contextlib

import jax
import jax.numpy as jnp
from jax import lax
from jax.experimental import pallas as pl
from jax.experimental.pallas import tpu as pltpu
from jax.sharding import PartitionSpec as P

F32 = jnp.float32
BF = jnp.bfloat16
NT = (((1,), (1,)), ((), ()))
MESH = pl.DeviceIdType.MESH
TABLES = 26
SIZES = (2,) * 13
NC = len(SIZES)
STARTS = tuple(sum(SIZES[:i]) for i in range(NC))
AHEAD = 3
GROUPS = (1,) * 13
CLOSE = {sum(GROUPS[:i + 1]) - 1: sum(GROUPS[:i]) for i in range(len(GROUPS))}
FLIP = 30
TOPK = -1


def lag_of(i, s):
    return LAG * s


LAG = 4
TOP_AT = -1
HOOKS = {"share": 8, "gather_z": 12, "gather_p": 14, "gather_c": 20}
RELAYED = NC - 1
TR = sum(SIZES[:RELAYED])
REST = 2 * TR + 3 * (TABLES - TR)
def scope(name):
    return contextlib.nullcontext()


def coords():
    r = lax.axis_index("rep")
    s = lax.axis_index("shard")
    return (s // 4) % 2 * 2 + r // 2, s % 4, s // 8, r % 2


def plane_peer(q):
    x, y, z, c = coords()
    xl = (x + q // 8) % 2
    xh = (x // 2 + q // 16) % 2
    yy = (y // 2 + q // 4) % 2 * 2 + (y + q // 2) % 2
    return (xl * 2 + (c + q) % 2, z * 8 + xh * 4 + yy)


def z_peer(d):
    return (lax.axis_index("rep"), (lax.axis_index("shard") + 8 * d + 64) % 64)


def rep_peer(i):
    r = lax.axis_index("rep")
    return ((r // 2 + i // 2) % 2 * 2 + (r + i) % 2, lax.axis_index("shard"))


def rcopy(src, dst, ss, rs, to):
    return pltpu.make_async_remote_copy(
        src_ref=src, dst_ref=dst, send_sem=ss, recv_sem=rs, device_id=to, device_id_type=MESH)


def wait_for(reg, sem):
    pltpu.make_async_copy(reg, reg, sem).wait()


def kernel(dense_h, pool_h, w_h, cot_h, idx_h, dgrad, topo, bias, tab,
           dense, pool, w, cot, idx, vt, g, gt, sl, blks, cols, keyt, krow, krv, kt,
           rows, rv, D, zr, fin, tb, tp, r0, s1, r2, pz,
           in_sem, s_send, k_send, s_recv, z_send, z_recv, a_send, a_recv, t_send, t_recv):
    x, y, z, c = coords()
    rep = lax.axis_index("rep")
    ins = [pltpu.make_async_copy(a, b, in_sem.at[i]) for i, (a, b) in enumerate(
        ((idx_h, idx), (pool_h, pool), (dense_h, dense), (cot_h, cot), (w_h, w)))]
    for cp in ins:
        cp.start()
    bar = pltpu.get_barrier_semaphore()
    with scope("bar"):
        for q in range(1, 32):
            pl.semaphore_signal(bar, 1, device_id=plane_peer(q), device_id_type=MESH)
        for d in range(1, 8):
            pl.semaphore_signal(bar, 1, device_id=z_peer(d), device_id_type=MESH)
    i0 = lax.broadcasted_iota(jnp.int32, (128, 128), 0)
    i1 = lax.broadcasted_iota(jnp.int32, (128, 128), 1)
    eye = (i0 == i1).astype(F32).astype(BF)
    one = jnp.float32(1)
    zero = jnp.float32(0)

    with scope("in0"):
        ins[0].wait()
    with scope("slots"):
        cols[...] = jnp.zeros_like(cols)
        keys, slots = [], []
        for l in range(2):
            row = idx[:, l, :]
            blk = row >> 6
            xx = ((row >> 10) & 1) * 2 + ((row >> 7) & 1)
            slot = ((xx ^ x) << 7) + ((((row >> 8) & 3) ^ y) << 5) + ((((row >> 6) & 1) ^ c) << 4)
            slot = slot + ((((row >> 11) - z) & 7) << 1)
            keys.append(((row & 63) + 1).astype(F32))
            slots.append(slot.astype(F32))
            cols[32 * l:32 * l + 26] = blk.astype(F32)
            blks[l] = blk.astype(F32)
        ct = cols[...].T
    base = slots

    def rank(tables):
        sub = lax.broadcasted_iota(jnp.int32, (8, 128), 0)
        lane = lax.broadcasted_iota(jnp.int32, (8, 128), 1)
        for t in tables:
            b0 = jnp.broadcast_to(blks[0, t:t + 1], (8, 128))
            b1 = jnp.broadcast_to(blks[1, t:t + 1], (8, 128))
            n0 = jnp.zeros((8, 128), F32)
            n1 = n0
            for k in range(16):
                c0 = jnp.broadcast_to(ct[8 * k:8 * k + 8, t:t + 1], (8, 128))
                c1 = jnp.broadcast_to(ct[8 * k:8 * k + 8, 32 + t:33 + t], (8, 128))
                lt = jnp.where(sub + 8 * k < lane, one, zero)
                n0 = n0 + jnp.where(c0 == b0, lt, zero)
                n1 = n1 + jnp.where(c0 == b1, one, zero) + jnp.where(c1 == b1, lt, zero)
            sl[0, t:t + 1] = base[0][t:t + 1] + jnp.sum(n0, axis=0, keepdims=True)
            sl[1, t:t + 1] = base[1][t:t + 1] + jnp.sum(n1, axis=0, keepdims=True)

    with scope("rank"):
        rank(range(SIZES[0]))

    def send_keys():
        for l in range(2):
            cols[32 * l:32 * l + 26] = sl[l]
            cols[64 + 32 * l:90 + 32 * l] = keys[l]
        ct = cols[...].T
        fl = lax.broadcasted_iota(jnp.int32, (8, 128), 1).astype(F32)
        lanes = [fl + jnp.float32(128 * b) for b in range(4)]
        keyt[...] = jnp.zeros_like(keyt)
        for t in range(TABLES):
            acc = [jnp.zeros((8, 128), F32)] * 4
            for k in range(16):
                col = [jnp.broadcast_to(ct[8 * k:8 * k + 8, 32 * j + t:32 * j + t + 1], (8, 128)) for j in range(4)]
                for b in range(4):
                    acc[b] = acc[b] + jnp.where(col[0] == lanes[b], col[2], zero) + jnp.where(col[1] == lanes[b], col[3], zero)
            for b in range(4):
                keyt[t:t + 1, 128 * b:128 * b + 128] = jnp.sum(acc[b], axis=0, keepdims=True)
        krow[...] = keyt[...].T.astype(BF)
        for q in range(1, 32):
            rcopy(krow.at[pl.ds(q * 16, 16)], krv.at[pl.ds(q * 16, 16)], k_send, s_recv.at[NC], plane_peer(q)).start()

    with scope("in1"):
        ins[1].wait()
        ins[2].wait()
    with scope("tr"):
        vt[0] = lax.dot_general(eye, dense[...], NT, preferred_element_type=F32)

        def tr(i, _):
            vt[i + 1] = lax.dot_general(eye, pool[i], NT, preferred_element_type=F32)
            return 0

        lax.fori_loop(0, TABLES, tr, 0, unroll=True)
    with scope("in3"):
        ins[3].wait()
        ins[4].wait()
    with scope("gt"):
        gt[0:479] = lax.dot_general(w[...], cot[...], NT, preferred_element_type=F32)
        gt[479:480] = jnp.zeros((1, 128), F32)
    with scope("barwait"):
        pl.semaphore_wait(bar, 38)

    def prow(a, b):
        hi = jnp.maximum(a, b)
        lo = jnp.minimum(a, b)
        return 128 + hi * (hi - 1) // 2 + lo

    def vg(i):
        acc = jnp.zeros((128, 128), F32)
        for j in range(27):
            p = jnp.where(i == j, 479, prow(i, jnp.int32(j)))
            acc = acc + gt[pl.ds(p, 1), :] * vt[j]
        return acc

    s512 = lax.broadcasted_iota(jnp.int32, (512, 128), 0).astype(F32)

    def compute(ch):
        t0, n = STARTS[ch], SIZES[ch]

        def table(t, _):
            v = vg(t + 1).astype(BF)
            p = jnp.where((s512 == sl[0, pl.ds(t, 1), :]) | (s512 == sl[1, pl.ds(t, 1), :]), one, zero)
            rows[t] = lax.dot_general(p.astype(BF), v, NT, preferred_element_type=F32).astype(BF)
            return 0

        lax.fori_loop(t0, t0 + n, table, 0, unroll=True)
        if ch in CLOSE:
            g0 = STARTS[CLOSE[ch]]
            n = t0 + n - g0
            for q in range(1, 32):
                rcopy(rows.at[pl.ds(g0, n), pl.ds(q * 16, 16)], rv.at[pl.ds(g0, n), pl.ds(q * 16, 16)],
                      s_send, s_recv.at[ch], plane_peer(q)).start()

    def dense_part():
        d0 = vg(jnp.int32(0)) + gt[0:128]
        dgrad[...] = lax.dot_general(eye, d0.astype(BF), NT, preferred_element_type=F32).astype(BF)

    def core_copy():
        return rcopy(tp.at[1 - c], r0, t_send.at[0], t_recv.at[0], rep_peer(1))

    def top_part():
        g[0:128] = vt[0]
        g[479:480] = jnp.ones((1, 128), F32)

        def gram(i, _):
            va = vt[i]
            for d in range(1, 14):
                j = i + d
                j = jnp.where(j >= 27, j - 27, j)
                g[pl.ds(prow(i, j), 1), :] = jnp.sum(va * vt[j], axis=0, keepdims=True)
            return 0

        lax.fori_loop(0, 27, gram, 0, unroll=3)
        gb = g[...].astype(BF)
        for i in range(2):
            tp[i, 0:480] = jnp.dot(gb, cot[:, 512 * i:512 * i + 512], preferred_element_type=F32).astype(BF)
            tp[i, 480:512] = jnp.zeros((32, 512), BF)
        core_copy().start()

    def top_sum():
        core_copy().wait_recv()
        for k in range(8):
            at = pl.ds(pl.multiple_of((z + k) % 8 * 64, 64), 64)
            v = (tp[c, at].astype(F32) + r0[at].astype(F32)).astype(BF)
            for b in range(4):
                D[TABLES + b, k] = v[:, 128 * b:128 * b + 128]
        zcopy(0, 1, NC).start()
        zcopy(1, 1, NC).start()

    def spot(ref, xx, yy):
        return ref.at[yy, pl.ds(pl.multiple_of(xx * 16, 16), 16)]

    def p_target(q):
        return (x // 2 + q // 8) % 2 * 2 + (x + q // 4) % 2, (y // 2 + q // 2) % 2 * 2 + (y + q) % 2

    def p_share(q):
        return rcopy(spot(s1, *p_target(q)), r2.at[q - 1], t_send.at[2], t_recv.at[2], plane_peer(q * 2))

    def z_gather(d):
        return rcopy(pz, tb.at[c, x * 4 + y, z], t_send.at[3], t_recv.at[3], z_peer(d))

    def p_gather(q):
        reg = tb.at[c, x * 4 + y]
        return rcopy(reg, reg, t_send.at[4], t_recv.at[4], plane_peer(q * 2))

    def core_gather():
        return rcopy(tb.at[c], tb.at[c], t_send.at[5], t_recv.at[5], rep_peer(1))

    def top_share():
        z_wait(4, NC)
        for b in range(4):
            e = TABLES + b
            s1[b] = D[e, 0].astype(F32) + zr[0, 3, e].astype(F32) + zr[1, 3, e].astype(F32)
        for q in range(1, 16):
            p_share(q).start()

    def top_gather_z():
        wait_for(r2, t_recv.at[2])
        a = spot(s1, x, y)[...]
        for i in range(15):
            a = a + r2[i]
        pz[...] = a.astype(BF)
        tb[c, x * 4 + y, z] = a.astype(BF)
        for d in range(1, 8):
            z_gather(d).start()

    def top_gather_p():
        wait_for(tb.at[0, 0, pl.ds(0, 7)], t_recv.at[3])
        for q in range(1, 16):
            p_gather(q).start()

    def top_gather_c():
        wait_for(tb.at[0, pl.ds(0, 15)], t_recv.at[4])
        core_gather().start()

    def span(ch):
        return (STARTS[ch], SIZES[ch]) if ch < NC else (TABLES, 4)

    def zcopy(dirn, step, ch):
        t0, n = span(ch)
        rel = (5 - step) if dirn == 0 else (3 + step)
        lo, sz = (32 * dirn, 32) if step == 1 else (0, 64)
        return rcopy(D.at[pl.ds(t0, n), rel, pl.ds(lo, sz)], zr.at[dirn, step - 1, pl.ds(t0, n), pl.ds(lo, sz)],
                     z_send, z_recv.at[step - 1, ch], z_peer(1 if dirn == 0 else -1))

    def z_wait(step, ch):
        t0, n = span(ch)
        reg = zr.at[0, 0, pl.ds(t0, n)] if step == 1 else zr.at[pl.ds(0, 2), step - 1, pl.ds(t0, n)]
        wait_for(reg, z_recv.at[step - 1, ch])

    def acopy(i, ch):
        t0, n = STARTS[ch], SIZES[ch]
        reg = fin.at[pl.ds(t0, n), pl.ds(pl.multiple_of(rep * 64, 64), 64)]
        got = a_recv.at[0] if i == 2 and ch < RELAYED else a_recv.at[1]
        return rcopy(reg, reg, a_send, got, rep_peer(i))

    def fwd():
        reg = fin.at[pl.ds(0, TR), pl.ds(pl.multiple_of((rep + 2) % 4 * 64, 64), 64)]
        return rcopy(reg, reg, a_send, a_recv.at[1], rep_peer(1))

    rowi = lax.broadcasted_iota(jnp.int32, (512, 512), 0).astype(F32)

    def gather_keys():
        wait_for(krv.at[pl.ds(16, 496)], s_recv.at[NC])
        krv[0:16] = krow[0:16]
        kk = lax.dot_general(eye, krv[...], NT, preferred_element_type=F32)
        zz = (((lax.broadcasted_iota(jnp.int32, (128, 512), 1) >> 1) & 7) << 6).astype(F32)
        kt[...] = jnp.where(kk > 0.5, kk - 1 + zz, -1.0)

    def gather_rows(ch):
        t0, n = STARTS[ch], SIZES[ch]
        for last, first in CLOSE.items():
            if first == ch:
                end = STARTS[last] + SIZES[last]
                wait_for(rv.at[pl.ds(t0, end - t0), pl.ds(16, 496)], s_recv.at[last])
        rv[t0:t0 + n, 0:16] = rows[t0:t0 + n, 0:16]

        def acc(t, _):
            oh = jnp.where(rowi == kt[pl.ds(t, 1), :], one, zero).astype(BF)
            D[t] = jnp.dot(oh, rv[t], preferred_element_type=F32).astype(BF).reshape(8, 64, 128)
            return 0

        lax.fori_loop(t0, t0 + n, acc, 0, unroll=True)
        zcopy(0, 1, ch).start()
        zcopy(1, 1, ch).start()

    def zstep(s, ch):
        t0, n = span(ch)
        z_wait(s, ch)
        for dirn in (0, 1):
            rel = (4 - s) if dirn == 0 else (4 + s)
            lo, sz = (32 * dirn, 32) if s == 1 else (0, 64)
            for e in range(t0, t0 + n):
                D[e, rel, lo:lo + sz] = (D[e, rel, lo:lo + sz].astype(F32) + zr[dirn, s - 1, e, lo:lo + sz].astype(F32)).astype(BF)
            zcopy(dirn, s + 1, ch).start()

    def finish(ch):
        t0, n = STARTS[ch], SIZES[ch]
        z_wait(4, ch)
        for e in range(t0, t0 + n):
            v = D[e, 0].astype(F32) + zr[0, 3, e].astype(F32) + zr[1, 3, e].astype(F32)
            fin[e, pl.ds(pl.multiple_of(rep * 64, 64), 64)] = v.astype(BF)
        acopy(1, ch).start()
        acopy(2, ch).start()
        if ch >= RELAYED:
            acopy(3, ch).start()

    def named(name, f, *args):
        with scope(name):
            f(*args)

    chain = list(range(NC))
    chain.insert(TOP_AT + 1, NC)
    named("comp", compute, 0)
    named("rank", rank, range(SIZES[0], TABLES))
    named("comp", compute, 1)
    named("keys", send_keys)
    named("comp", compute, 2)
    if TOPK < 0:
        named("top", top_part)
    made = AHEAD
    extra = {v: k for k, v in HOOKS.items()}
    acts = {"share": top_share, "gather_z": top_gather_z, "gather_p": top_gather_p, "gather_c": top_gather_c}
    halves = {}
    for i, ch in enumerate(chain):
        for s in (1, 2, 3, 4):
            halves.setdefault(2 * i + lag_of(i, s), []).append((i, s, ch))
    n = max(max(halves), 2 * max(extra) + 1) + 1
    for h in range(n):
        k = h // 2
        if h % 2 == 0:
            if made < NC:
                named("comp", compute, made)
                made += 1
            elif made == NC:
                named("dense", dense_part)
                made += 1
        for i, s, ch in sorted(halves.get(h, []), reverse=h >= FLIP):
            if s < 4:
                named("zs%d_%d" % (s, ch), zstep, s, ch)
            elif ch < NC:
                named("fin%d" % ch, finish, ch)
        if h % 2 == 0 and k < len(chain):
            if chain[k] == NC:
                named("tsum", top_sum)
            else:
                if chain[k] == 0:
                    named("gkeys", gather_keys)
                named("gath%d" % chain[k], gather_rows, chain[k])
        if h == 2 * TOPK:
            named("top", top_part)
        if h % 2 == 1 and k in extra:
            named(extra[k], acts[extra[k]])
    with scope("fwd"):
        wait_for(fin.at[pl.ds(0, TR), pl.ds(0, 64)], a_recv.at[0])
        fwd().start()
    with scope("topw"):
        core_gather().wait_recv()
        for cc in range(2):
            for xx in range(4):
                for yy in range(4):
                    for zz in range(8):
                        r, q = zz * 64 + xx * 16, cc * 512 + yy * 128
                        if r < 464:
                            topo[r:r + 16, q:q + 128] = tb[cc, xx * 4 + yy, zz].astype(F32)
                        elif r == 464:
                            v = tb[cc, xx * 4 + yy, zz].astype(F32)
                            topo[r:r + 15, q:q + 128] = v[0:15]
                            bias[q // 128:q // 128 + 1] = v[15:16]
    with scope("tabw"):
        wait_for(zr.at[0, pl.ds(0, 2), pl.ds(0, REST // 2)], a_recv.at[1])
        tab[...] = fin[...].astype(F32)
    with scope("drain"):
        wait_for(fin.at[pl.ds(0, TABLES), pl.ds(0, 192)], a_send)
        wait_for(rows.at[pl.ds(0, TABLES), pl.ds(16, 496)], s_send)
        wait_for(D.at[pl.ds(0, TABLES + 4), pl.ds(0, 7)], z_send)
        wait_for(krow.at[pl.ds(16, 496)], k_send)
        core_copy().wait_send()
        wait_for(r2, t_send.at[2])
        wait_for(tb.at[0, 0, pl.ds(0, 7)], t_send.at[3])
        wait_for(tb.at[0, pl.ds(0, 15)], t_send.at[4])
        core_gather().wait_send()


def fused_call(dense, pool, w, cot, idx, cid=1, name="fused"):
    vm = pl.BlockSpec(memory_space=pltpu.VMEM)
    hbm = pl.BlockSpec(memory_space=pltpu.HBM)
    dma = pltpu.SemaphoreType.DMA
    V = pltpu.VMEM
    E = TABLES + 4
    return pl.pallas_call(
        kernel,
        out_shape=(
            jax.ShapeDtypeStruct((128, 128), BF),
            jax.ShapeDtypeStruct((479, 1024), F32),
            jax.ShapeDtypeStruct((8, 128), F32),
            jax.ShapeDtypeStruct((TABLES, 256, 128), F32),
        ),
        in_specs=[hbm] * 5,
        out_specs=(vm,) * 4,
        scratch_shapes=[
            V((128, 128), BF), V((TABLES, 128, 128), BF), V((479, 1024), BF), V((128, 1024), BF), V((TABLES, 2, 128), jnp.int32),
            V((27, 128, 128), F32), V((480, 128), F32), V((480, 128), F32), V((2, TABLES, 128), F32), V((2, TABLES, 128), F32), V((128, 128), F32),
            V((128, 512), F32), V((512, 128), BF), V((512, 128), BF), V((128, 512), F32),
            V((TABLES, 512, 128), BF), V((TABLES, 512, 128), BF), V((E, 8, 64, 128), BF), V((2, 4, E, 64, 128), BF),
            V((TABLES, 256, 128), BF),
            V((2, 16, 8, 16, 128), BF), V((2, 512, 512), BF), V((512, 512), BF), V((4, 64, 128), F32), V((15, 16, 128), F32), V((16, 128), BF),
            dma((5,)), dma(()), dma(()), dma((NC + 1,)), dma(()), dma((4, NC + 1)), dma(()), dma((2,)), dma((6,)), dma((6,)),
        ],
        compiler_params=pltpu.CompilerParams(collective_id=cid, has_side_effects=True, vmem_limit_bytes=40 * 2**20),
        name=name,
    )(*[pltpu.with_memory_space_constraint(a, pltpu.HBM) for a in (dense, pool, w, cot, idx)])


def result_kernel(dgrad, topo, bias, tab, dgrad_o, topo_o, bias_o, tab_o, sem):
    for i in range(0, TABLES, 2):
        pltpu.make_async_copy(tab.at[pl.ds(i, 2)], tab_o.at[pl.ds(i, 2)], sem.at[0]).start()
    for i, n in ((0, 120), (120, 120), (240, 120), (360, 119)):
        pltpu.make_async_copy(topo.at[pl.ds(i, n)], topo_o.at[pl.ds(i, n)], sem.at[1]).start()
    pltpu.make_async_copy(dgrad, dgrad_o, sem.at[2]).start()
    pltpu.make_async_copy(bias, bias_o, sem.at[3]).start()
    for i, (a, b) in enumerate(((tab, tab_o), (topo, topo_o), (dgrad, dgrad_o), (bias, bias_o))):
        pltpu.make_async_copy(a, b, sem.at[i]).wait()


def result_call(*arrays):
    vm = pl.BlockSpec(memory_space=pltpu.VMEM)
    hbm = pl.BlockSpec(memory_space=pltpu.HBM)
    return pl.pallas_call(
        result_kernel, out_shape=tuple(jax.ShapeDtypeStruct(a.shape, a.dtype) for a in arrays),
        in_specs=[vm] * 4, out_specs=(hbm,) * 4, scratch_shapes=[pltpu.SemaphoreType.DMA((4,))],
        compiler_params=pltpu.CompilerParams(vmem_limit_bytes=2**20), name="result")(*arrays)


def on_device(dense_out, pooled, top_weight, top_cotangent, indices):
    dgrad, top, bias, table = fused_call(
        dense_out, jnp.transpose(pooled, (1, 0, 2)), top_weight, top_cotangent, jnp.transpose(indices, (1, 2, 0)))
    dgrad, top, bias, table = result_call(dgrad, top, bias, table)
    return dgrad, top, bias.reshape(1024), table


def solution(mesh):
    both = P(("rep", "shard"))
    return jax.shard_map(
        on_device, mesh=mesh, in_specs=(both, both, P(), both, both),
        out_specs=(both, P(), P(), P(None, "shard", None)), check_vma=False)
```

```python
import contextlib

import jax
import jax.numpy as jnp
from jax import lax
from jax.experimental import pallas as pl
from jax.experimental.pallas import tpu as pltpu
from jax.sharding import PartitionSpec as P

F32 = jnp.float32
BF = jnp.bfloat16
NT = (((1,), (1,)), ((), ()))
MESH = pl.DeviceIdType.MESH
TABLES = 26
SIZES = (2,) * 13
NC = len(SIZES)
STARTS = tuple(sum(SIZES[:i]) for i in range(NC))
AHEAD = 3
GROUPS = (1,) * 13
CLOSE = {sum(GROUPS[:i + 1]) - 1: sum(GROUPS[:i]) for i in range(len(GROUPS))}
FLIP = 27
TOPK = -1


def lag_of(i, s):
    return LAG * s


LAG = 4
TOP_AT = -1
HOOKS = {"share": 8, "gather_z": 12, "gather_p": 14, "gather_c": 21}
RELAYED = NC - 1
TR = sum(SIZES[:RELAYED])
REST = 2 * TR + 3 * (TABLES - TR)
def scope(name):
    return contextlib.nullcontext()


def coords():
    r = lax.axis_index("rep")
    s = lax.axis_index("shard")
    return (s // 4) % 2 * 2 + r // 2, s % 4, s // 8, r % 2


def plane_peer(q):
    x, y, z, c = coords()
    xl = (x + q // 8) % 2
    xh = (x // 2 + q // 16) % 2
    yy = (y // 2 + q // 4) % 2 * 2 + (y + q // 2) % 2
    return (xl * 2 + (c + q) % 2, z * 8 + xh * 4 + yy)


def z_peer(d):
    return (lax.axis_index("rep"), (lax.axis_index("shard") + 8 * d + 64) % 64)


def rep_peer(i):
    r = lax.axis_index("rep")
    return ((r // 2 + i // 2) % 2 * 2 + (r + i) % 2, lax.axis_index("shard"))


def rcopy(src, dst, ss, rs, to):
    return pltpu.make_async_remote_copy(
        src_ref=src, dst_ref=dst, send_sem=ss, recv_sem=rs, device_id=to, device_id_type=MESH)


def wait_for(reg, sem):
    pltpu.make_async_copy(reg, reg, sem).wait()


def kernel(dense_h, pool_h, w_h, cot_h, idx_h, dgrad, topo, bias, tab,
           dense, pool, w, cot, idx, vt, g, gt, sl, blks, cols, keyt, krow, krv, kt,
           rows, rv, D, zr, fin, tb, tp, r0, s1, r2, pz,
           in_sem, s_send, k_send, s_recv, z_send, z_recv, a_send, a_recv, t_send, t_recv):
    x, y, z, c = coords()
    rep = lax.axis_index("rep")
    ins = [pltpu.make_async_copy(a, b, in_sem.at[i]) for i, (a, b) in enumerate(
        ((idx_h, idx), (pool_h, pool), (dense_h, dense), (cot_h, cot), (w_h, w)))]
    for cp in ins:
        cp.start()
    bar = pltpu.get_barrier_semaphore()
    with scope("bar"):
        for q in range(1, 32):
            pl.semaphore_signal(bar, 1, device_id=plane_peer(q), device_id_type=MESH)
        for d in range(1, 8):
            pl.semaphore_signal(bar, 1, device_id=z_peer(d), device_id_type=MESH)
    i0 = lax.broadcasted_iota(jnp.int32, (128, 128), 0)
    i1 = lax.broadcasted_iota(jnp.int32, (128, 128), 1)
    eye = (i0 == i1).astype(F32).astype(BF)
    one = jnp.float32(1)
    zero = jnp.float32(0)

    with scope("in0"):
        ins[0].wait()
    with scope("slots"):
        cols[...] = jnp.zeros_like(cols)
        keys, slots = [], []
        for l in range(2):
            row = idx[:, l, :]
            blk = row >> 6
            xx = ((row >> 10) & 1) * 2 + ((row >> 7) & 1)
            slot = ((xx ^ x) << 7) + ((((row >> 8) & 3) ^ y) << 5) + ((((row >> 6) & 1) ^ c) << 4)
            slot = slot + ((((row >> 11) - z) & 7) << 1)
            keys.append(((row & 63) + 1).astype(F32))
            slots.append(slot.astype(F32))
            cols[32 * l:32 * l + 26] = blk.astype(F32)
            blks[l] = blk.astype(F32)
        ct = cols[...].T
    base = slots

    def rank(tables):
        sub = lax.broadcasted_iota(jnp.int32, (8, 128), 0)
        lane = lax.broadcasted_iota(jnp.int32, (8, 128), 1)
        for t in tables:
            b0 = jnp.broadcast_to(blks[0, t:t + 1], (8, 128))
            b1 = jnp.broadcast_to(blks[1, t:t + 1], (8, 128))
            n0 = jnp.zeros((8, 128), F32)
            n1 = n0
            for k in range(16):
                c0 = jnp.broadcast_to(ct[8 * k:8 * k + 8, t:t + 1], (8, 128))
                c1 = jnp.broadcast_to(ct[8 * k:8 * k + 8, 32 + t:33 + t], (8, 128))
                lt = jnp.where(sub + 8 * k < lane, one, zero)
                n0 = n0 + jnp.where(c0 == b0, lt, zero)
                n1 = n1 + jnp.where(c0 == b1, one, zero) + jnp.where(c1 == b1, lt, zero)
            sl[0, t:t + 1] = base[0][t:t + 1] + jnp.sum(n0, axis=0, keepdims=True)
            sl[1, t:t + 1] = base[1][t:t + 1] + jnp.sum(n1, axis=0, keepdims=True)

    with scope("rank"):
        rank(range(SIZES[0]))

    def send_keys():
        for l in range(2):
            cols[32 * l:32 * l + 26] = sl[l]
            cols[64 + 32 * l:90 + 32 * l] = keys[l]
        ct = cols[...].T
        fl = lax.broadcasted_iota(jnp.int32, (8, 128), 1).astype(F32)
        lanes = [fl + jnp.float32(128 * b) for b in range(4)]
        keyt[...] = jnp.zeros_like(keyt)
        for t in range(TABLES):
            acc = [jnp.zeros((8, 128), F32)] * 4
            for k in range(16):
                col = [jnp.broadcast_to(ct[8 * k:8 * k + 8, 32 * j + t:32 * j + t + 1], (8, 128)) for j in range(4)]
                for b in range(4):
                    acc[b] = acc[b] + jnp.where(col[0] == lanes[b], col[2], zero) + jnp.where(col[1] == lanes[b], col[3], zero)
            for b in range(4):
                keyt[t:t + 1, 128 * b:128 * b + 128] = jnp.sum(acc[b], axis=0, keepdims=True)
        krow[...] = keyt[...].T.astype(BF)
        for q in range(1, 32):
            rcopy(krow.at[pl.ds(q * 16, 16)], krv.at[pl.ds(q * 16, 16)], k_send, s_recv.at[NC], plane_peer(q)).start()

    with scope("in1"):
        ins[1].wait()
        ins[2].wait()
    with scope("tr"):
        vt[0] = lax.dot_general(eye, dense[...], NT, preferred_element_type=F32)

        def tr(i, _):
            vt[i + 1] = lax.dot_general(eye, pool[i], NT, preferred_element_type=F32)
            return 0

        lax.fori_loop(0, TABLES, tr, 0, unroll=True)
    with scope("in3"):
        ins[3].wait()
        ins[4].wait()
    with scope("gt"):
        gt[0:479] = lax.dot_general(w[...], cot[...], NT, preferred_element_type=F32)
        gt[479:480] = jnp.zeros((1, 128), F32)
    with scope("barwait"):
        pl.semaphore_wait(bar, 38)

    def prow(a, b):
        hi = jnp.maximum(a, b)
        lo = jnp.minimum(a, b)
        return 128 + hi * (hi - 1) // 2 + lo

    def vg(i):
        acc = jnp.zeros((128, 128), F32)
        for j in range(27):
            p = jnp.where(i == j, 479, prow(i, jnp.int32(j)))
            acc = acc + gt[pl.ds(p, 1), :] * vt[j]
        return acc

    s512 = lax.broadcasted_iota(jnp.int32, (512, 128), 0).astype(F32)

    def compute(ch):
        t0, n = STARTS[ch], SIZES[ch]

        def table(t, _):
            v = vg(t + 1).astype(BF)
            p = jnp.where((s512 == sl[0, pl.ds(t, 1), :]) | (s512 == sl[1, pl.ds(t, 1), :]), one, zero)
            rows[t] = lax.dot_general(p.astype(BF), v, NT, preferred_element_type=F32).astype(BF)
            return 0

        lax.fori_loop(t0, t0 + n, table, 0, unroll=True)
        if ch in CLOSE:
            g0 = STARTS[CLOSE[ch]]
            n = t0 + n - g0
            for q in range(1, 32):
                rcopy(rows.at[pl.ds(g0, n), pl.ds(q * 16, 16)], rv.at[pl.ds(g0, n), pl.ds(q * 16, 16)],
                      s_send, s_recv.at[ch], plane_peer(q)).start()

    def dense_part():
        d0 = vg(jnp.int32(0)) + gt[0:128]
        dgrad[...] = lax.dot_general(eye, d0.astype(BF), NT, preferred_element_type=F32).astype(BF)

    def core_copy():
        return rcopy(tp.at[1 - c], r0, t_send.at[0], t_recv.at[0], rep_peer(1))

    def top_part():
        g[0:128] = vt[0]
        g[479:480] = jnp.ones((1, 128), F32)

        def gram(i, _):
            va = vt[i]
            for d in range(1, 14):
                j = i + d
                j = jnp.where(j >= 27, j - 27, j)
                g[pl.ds(prow(i, j), 1), :] = jnp.sum(va * vt[j], axis=0, keepdims=True)
            return 0

        lax.fori_loop(0, 27, gram, 0, unroll=9)
        gb = g[...].astype(BF)
        for i in range(2):
            tp[i, 0:480] = jnp.dot(gb, cot[:, 512 * i:512 * i + 512], preferred_element_type=F32).astype(BF)
            tp[i, 480:512] = jnp.zeros((32, 512), BF)
        core_copy().start()

    def top_sum():
        core_copy().wait_recv()
        for k in range(8):
            at = pl.ds(pl.multiple_of((z + k) % 8 * 64, 64), 64)
            v = (tp[c, at].astype(F32) + r0[at].astype(F32)).astype(BF)
            for b in range(4):
                D[TABLES + b, k] = v[:, 128 * b:128 * b + 128]
        zcopy(0, 1, NC).start()
        zcopy(1, 1, NC).start()

    def spot(ref, xx, yy):
        return ref.at[yy, pl.ds(pl.multiple_of(xx * 16, 16), 16)]

    def p_target(q):
        return (x // 2 + q // 8) % 2 * 2 + (x + q // 4) % 2, (y // 2 + q // 2) % 2 * 2 + (y + q) % 2

    def p_share(q):
        return rcopy(spot(s1, *p_target(q)), r2.at[q - 1], t_send.at[2], t_recv.at[2], plane_peer(q * 2))

    def z_gather(d):
        return rcopy(pz, tb.at[c, x * 4 + y, z], t_send.at[3], t_recv.at[3], z_peer(d))

    def p_gather(q):
        reg = tb.at[c, x * 4 + y]
        return rcopy(reg, reg, t_send.at[4], t_recv.at[4], plane_peer(q * 2))

    def core_gather():
        return rcopy(tb.at[c], tb.at[c], t_send.at[5], t_recv.at[5], rep_peer(1))

    def top_share():
        z_wait(4, NC)
        for b in range(4):
            e = TABLES + b
            s1[b] = D[e, 0].astype(F32) + zr[0, 3, e].astype(F32) + zr[1, 3, e].astype(F32)
        for q in range(1, 16):
            p_share(q).start()

    def top_gather_z():
        wait_for(r2, t_recv.at[2])
        a = spot(s1, x, y)[...]
        for i in range(15):
            a = a + r2[i]
        pz[...] = a.astype(BF)
        tb[c, x * 4 + y, z] = a.astype(BF)
        for d in range(1, 8):
            z_gather(d).start()

    def top_gather_p():
        wait_for(tb.at[0, 0, pl.ds(0, 7)], t_recv.at[3])
        for q in range(1, 16):
            p_gather(q).start()

    def top_gather_c():
        wait_for(tb.at[0, pl.ds(0, 15)], t_recv.at[4])
        core_gather().start()

    def span(ch):
        return (STARTS[ch], SIZES[ch]) if ch < NC else (TABLES, 4)

    def zcopy(dirn, step, ch):
        t0, n = span(ch)
        rel = (5 - step) if dirn == 0 else (3 + step)
        lo, sz = (32 * dirn, 32) if step == 1 else (0, 64)
        return rcopy(D.at[pl.ds(t0, n), rel, pl.ds(lo, sz)], zr.at[dirn, step - 1, pl.ds(t0, n), pl.ds(lo, sz)],
                     z_send, z_recv.at[step - 1, ch], z_peer(1 if dirn == 0 else -1))

    def z_wait(step, ch):
        t0, n = span(ch)
        reg = zr.at[0, 0, pl.ds(t0, n)] if step == 1 else zr.at[pl.ds(0, 2), step - 1, pl.ds(t0, n)]
        wait_for(reg, z_recv.at[step - 1, ch])

    def acopy(i, ch):
        t0, n = STARTS[ch], SIZES[ch]
        reg = fin.at[pl.ds(t0, n), pl.ds(pl.multiple_of(rep * 64, 64), 64)]
        got = a_recv.at[0] if i == 2 and ch < RELAYED else a_recv.at[1]
        return rcopy(reg, reg, a_send, got, rep_peer(i))

    def fwd():
        reg = fin.at[pl.ds(0, TR), pl.ds(pl.multiple_of((rep + 2) % 4 * 64, 64), 64)]
        return rcopy(reg, reg, a_send, a_recv.at[1], rep_peer(1))

    rowi = lax.broadcasted_iota(jnp.int32, (512, 512), 0).astype(F32)

    def gather_keys():
        wait_for(krv.at[pl.ds(16, 496)], s_recv.at[NC])
        krv[0:16] = krow[0:16]
        kk = lax.dot_general(eye, krv[...], NT, preferred_element_type=F32)
        zz = (((lax.broadcasted_iota(jnp.int32, (128, 512), 1) >> 1) & 7) << 6).astype(F32)
        kt[...] = jnp.where(kk > 0.5, kk - 1 + zz, -1.0)

    def gather_rows(ch):
        t0, n = STARTS[ch], SIZES[ch]
        for last, first in CLOSE.items():
            if first == ch:
                end = STARTS[last] + SIZES[last]
                wait_for(rv.at[pl.ds(t0, end - t0), pl.ds(16, 496)], s_recv.at[last])
        rv[t0:t0 + n, 0:16] = rows[t0:t0 + n, 0:16]

        def acc(t, _):
            oh = jnp.where(rowi == kt[pl.ds(t, 1), :], one, zero).astype(BF)
            D[t] = jnp.dot(oh, rv[t], preferred_element_type=F32).astype(BF).reshape(8, 64, 128)
            return 0

        lax.fori_loop(t0, t0 + n, acc, 0, unroll=True)
        zcopy(0, 1, ch).start()
        zcopy(1, 1, ch).start()

    def zstep(s, ch):
        t0, n = span(ch)
        z_wait(s, ch)
        for dirn in (0, 1):
            rel = (4 - s) if dirn == 0 else (4 + s)
            lo, sz = (32 * dirn, 32) if s == 1 else (0, 64)
            for e in range(t0, t0 + n):
                D[e, rel, lo:lo + sz] = (D[e, rel, lo:lo + sz].astype(F32) + zr[dirn, s - 1, e, lo:lo + sz].astype(F32)).astype(BF)
            zcopy(dirn, s + 1, ch).start()

    def finish(ch):
        t0, n = STARTS[ch], SIZES[ch]
        z_wait(4, ch)
        for e in range(t0, t0 + n):
            v = D[e, 0].astype(F32) + zr[0, 3, e].astype(F32) + zr[1, 3, e].astype(F32)
            fin[e, pl.ds(pl.multiple_of(rep * 64, 64), 64)] = v.astype(BF)
        acopy(1, ch).start()
        acopy(2, ch).start()
        if ch >= RELAYED:
            acopy(3, ch).start()

    def named(name, f, *args):
        with scope(name):
            f(*args)

    chain = list(range(NC))
    chain.insert(TOP_AT + 1, NC)
    named("comp", compute, 0)
    named("rank", rank, range(SIZES[0], TABLES))
    named("comp", compute, 1)
    named("keys", send_keys)
    named("comp", compute, 2)
    if TOPK < 0:
        named("top", top_part)
    made = AHEAD
    extra = {v: k for k, v in HOOKS.items()}
    acts = {"share": top_share, "gather_z": top_gather_z, "gather_p": top_gather_p, "gather_c": top_gather_c}
    halves = {}
    for i, ch in enumerate(chain):
        for s in (1, 2, 3, 4):
            halves.setdefault(2 * i + lag_of(i, s), []).append((i, s, ch))
    n = max(max(halves), 2 * max(extra) + 1) + 1
    for h in range(n):
        k = h // 2
        if h % 2 == 0:
            if made < NC:
                named("comp", compute, made)
                made += 1
            elif made == NC:
                named("dense", dense_part)
                made += 1
        for i, s, ch in sorted(halves.get(h, []), reverse=h >= FLIP):
            if s < 4:
                named("zs%d_%d" % (s, ch), zstep, s, ch)
            elif ch < NC:
                named("fin%d" % ch, finish, ch)
        if h % 2 == 0 and k < len(chain):
            if chain[k] == NC:
                named("tsum", top_sum)
            else:
                if chain[k] == 0:
                    named("gkeys", gather_keys)
                named("gath%d" % chain[k], gather_rows, chain[k])
        if h == 2 * TOPK:
            named("top", top_part)
        if h % 2 == 1 and k in extra:
            named(extra[k], acts[extra[k]])
    with scope("fwd"):
        wait_for(fin.at[pl.ds(0, TR), pl.ds(0, 64)], a_recv.at[0])
        fwd().start()
    with scope("topw"):
        core_gather().wait_recv()
        for cc in range(2):
            for xx in range(4):
                for yy in range(4):
                    for zz in range(8):
                        r, q = zz * 64 + xx * 16, cc * 512 + yy * 128
                        if r < 464:
                            topo[r:r + 16, q:q + 128] = tb[cc, xx * 4 + yy, zz].astype(F32)
                        elif r == 464:
                            v = tb[cc, xx * 4 + yy, zz].astype(F32)
                            topo[r:r + 15, q:q + 128] = v[0:15]
                            bias[q // 128:q // 128 + 1] = v[15:16]
    with scope("tabw"):
        wait_for(zr.at[0, pl.ds(0, 2), pl.ds(0, REST // 2)], a_recv.at[1])
        tab[...] = fin[...].astype(F32)
    with scope("drain"):
        wait_for(fin.at[pl.ds(0, TABLES), pl.ds(0, 192)], a_send)
        wait_for(rows.at[pl.ds(0, TABLES), pl.ds(16, 496)], s_send)
        wait_for(D.at[pl.ds(0, TABLES + 4), pl.ds(0, 7)], z_send)
        wait_for(krow.at[pl.ds(16, 496)], k_send)
        core_copy().wait_send()
        wait_for(r2, t_send.at[2])
        wait_for(tb.at[0, 0, pl.ds(0, 7)], t_send.at[3])
        wait_for(tb.at[0, pl.ds(0, 15)], t_send.at[4])
        core_gather().wait_send()


def fused_call(dense, pool, w, cot, idx, cid=1, name="fused"):
    vm = pl.BlockSpec(memory_space=pltpu.VMEM)
    hbm = pl.BlockSpec(memory_space=pltpu.HBM)
    dma = pltpu.SemaphoreType.DMA
    V = pltpu.VMEM
    E = TABLES + 4
    return pl.pallas_call(
        kernel,
        out_shape=(
            jax.ShapeDtypeStruct((128, 128), BF),
            jax.ShapeDtypeStruct((479, 1024), F32),
            jax.ShapeDtypeStruct((8, 128), F32),
            jax.ShapeDtypeStruct((TABLES, 256, 128), F32),
        ),
        in_specs=[hbm] * 5,
        out_specs=(vm,) * 4,
        scratch_shapes=[
            V((128, 128), BF), V((TABLES, 128, 128), BF), V((479, 1024), BF), V((128, 1024), BF), V((TABLES, 2, 128), jnp.int32),
            V((27, 128, 128), F32), V((480, 128), F32), V((480, 128), F32), V((2, TABLES, 128), F32), V((2, TABLES, 128), F32), V((128, 128), F32),
            V((128, 512), F32), V((512, 128), BF), V((512, 128), BF), V((128, 512), F32),
            V((TABLES, 512, 128), BF), V((TABLES, 512, 128), BF), V((E, 8, 64, 128), BF), V((2, 4, E, 64, 128), BF),
            V((TABLES, 256, 128), BF),
            V((2, 16, 8, 16, 128), BF), V((2, 512, 512), BF), V((512, 512), BF), V((4, 64, 128), F32), V((15, 16, 128), F32), V((16, 128), BF),
            dma((5,)), dma(()), dma(()), dma((NC + 1,)), dma(()), dma((4, NC + 1)), dma(()), dma((2,)), dma((6,)), dma((6,)),
        ],
        compiler_params=pltpu.CompilerParams(collective_id=cid, has_side_effects=True, vmem_limit_bytes=40 * 2**20),
        name=name,
    )(*[pltpu.with_memory_space_constraint(a, pltpu.HBM) for a in (dense, pool, w, cot, idx)])


def result_kernel(dgrad, topo, bias, tab, dgrad_o, topo_o, bias_o, tab_o, sem):
    pairs = [(tab.at[pl.ds(i, 2)], tab_o.at[pl.ds(i, 2)]) for i in range(0, TABLES, 2)]
    pairs += [(topo.at[pl.ds(i, 120)], topo_o.at[pl.ds(i, 120)]) for i in (0, 120, 240)]
    pairs += [(topo.at[pl.ds(360, 119)], topo_o.at[pl.ds(360, 119)]), (dgrad, dgrad_o), (bias, bias_o)]
    copies = [pltpu.make_async_copy(a, b, sem.at[i]) for i, (a, b) in enumerate(pairs)]
    for cp in copies:
        cp.start()
    for cp in copies:
        cp.wait()


def result_call(*arrays):
    vm = pl.BlockSpec(memory_space=pltpu.VMEM)
    hbm = pl.BlockSpec(memory_space=pltpu.HBM)
    return pl.pallas_call(
        result_kernel, out_shape=tuple(jax.ShapeDtypeStruct(a.shape, a.dtype) for a in arrays),
        in_specs=[vm] * 4, out_specs=(hbm,) * 4, scratch_shapes=[pltpu.SemaphoreType.DMA((19,))],
        compiler_params=pltpu.CompilerParams(vmem_limit_bytes=2**20), name="result")(*arrays)


def on_device(dense_out, pooled, top_weight, top_cotangent, indices):
    dgrad, top, bias, table = fused_call(
        dense_out, jnp.transpose(pooled, (1, 0, 2)), top_weight, top_cotangent, jnp.transpose(indices, (1, 2, 0)))
    dgrad, top, bias, table = result_call(dgrad, top, bias, table)
    return dgrad, top, bias.reshape(1024), table


def solution(mesh):
    both = P(("rep", "shard"))
    return jax.shard_map(
        on_device, mesh=mesh, in_specs=(both, both, P(), both, both),
        out_specs=(both, P(), P(), P(None, "shard", None)), check_vma=False)
```
